256 devices in a mesh: vert: 256 (over z, x, y, core).
Axes of the slice: x: 4, y: 4, z: 8, core: 2. Of those that a mesh axis runs over, the one named last changes fastest.
Arguments:
- feats: bfloat16 [524288, 128], P('vert'), may hold values from -6 to 6
- w_self: bfloat16 [128, 256], replicated, may hold values from -0.5 to 0.5
- w_neigh: bfloat16 [128, 256], replicated, may hold values from -0.5 to 0.5
- bias: float32 [256], replicated, may hold values from -0.6 to 0.6
- cotangent: bfloat16 [524288, 256], P('vert'), may hold values from -24 to 24
- send_rows: int32 [256, 256, 8], P('vert'), may hold values from 0 to 2047
- hub_ids: int32 [368], replicated, may hold values from 0 to 524287, as said below
- edge_src: int32 [256, 16384], P('vert'), may hold values from 0 to 4463, as said below
- edge_dst: int32 [256, 16384], P('vert'), may hold values from 0 to 2047, never falling along the last dimension, each value on 1 to 64 neighbouring positions
- edge_count: int32 [256], P('vert'), may hold values from 1 to 16384, 1677721 in all
Outputs:
- output: bfloat16 [524288, 256], P('vert')
- grad_feats: bfloat16 [524288, 128], P('vert')
- grad_w_self: float32 [128, 256], replicated
- grad_w_neigh: float32 [128, 256], replicated
- grad_bias: float32 [256], replicated
The draws below stay inside these ranges and needn't reach their ends.
Inputs may be any that keep to these rules, and one draw needn't show every extreme that they name: edge_src[d, e] indexes block d's source table: values below 2048 are own rows, values from 2048 to 4095 are halo slots (owner p = (value - 2048) // 8, slot c = (value - 2048) % 8), higher values are hubs (index value - 2048 - 256*8 into hub_ids). hub_ids is strictly ascending; no device's id range holds more than 8 hubs, some device's range holds exactly 8, and every device's range holds at least one.
All inputs are finite; a program needn't handle non-finite values.
Results may differ from the reference program's by a relative error of at most 0.0055.
Values may be sent and summed in bfloat16 or wider, within the bound.
A program may use at most 64 MiB of HBM per device.

```python
import math
import jax
import jax.numpy as jnp
import numpy as np
from jax import lax

F_IN = 128
F_OUT = 256
V_DEV = 2048
C_REST = 8
HUB_MOST = 8
DEG_MOST = 64
E_DEV = 16384
VERTICES = 524288
HUBS = 368
N_VERT = 256


def pick_places(place_key):
    return jax.random.permutation(place_key, V_DEV)[:HUB_MOST]


def draw_hub_ids(key, part):
    base_key = jax.random.fold_in(key, 23)
    order_key, place_key = jax.random.split(base_key)
    owners = jnp.arange(N_VERT, dtype=jnp.int32)
    ranking = jax.random.permutation(order_key, N_VERT).astype(jnp.int32)
    heavy_count = N_VERT // 16
    hub_counts = jnp.where(ranking < heavy_count, HUB_MOST, 1)
    place_keys = jax.random.split(place_key, N_VERT)
    picked = jax.vmap(pick_places)(place_keys).astype(jnp.int32)
    column = jnp.arange(HUB_MOST, dtype=jnp.int32)
    global_ids = owners[:, None] * V_DEV + picked
    marked = jnp.where(column[None, :] < hub_counts[:, None], global_ids, N_VERT * V_DEV)
    return jnp.sort(marked.reshape(-1))[:HUBS].astype(jnp.int32)


def draw_edge_src(key, part):
    base_key = jax.random.fold_in(key, 41)
    key_list = jax.random.split(base_key, 6)
    grid_shape = (N_VERT, E_DEV)
    category = jax.random.randint(key_list[0], grid_shape, 0, 8)
    local_pick = jax.random.randint(key_list[1], grid_shape, 0, V_DEV)
    halo_pick = V_DEV + jax.random.randint(key_list[2], grid_shape, 0, N_VERT * C_REST)
    draw_one = jax.random.randint(key_list[3], grid_shape, 0, HUBS)
    draw_two = jax.random.randint(key_list[4], grid_shape, 0, HUBS)
    uniform_hub = jax.random.randint(key_list[5], grid_shape, 0, HUBS)
    hub_base = V_DEV + N_VERT * C_REST
    hub_pick = hub_base + jnp.where(category == 6, jnp.minimum(draw_one, draw_two), uniform_hub)
    chosen = jnp.where(category < 3, local_pick, jnp.where(category < 6, halo_pick, hub_pick))
    return chosen.astype(jnp.int32)


def place_ends(array, own_key, low, high):
    spot = [jax.random.randint(jax.random.fold_in(own_key, axis), (), 0, length) for axis, length in enumerate(array.shape)]
    widest = array.shape.index(max(array.shape))
    neighbour = spot[:widest] + [(spot[widest] + 1) % array.shape[widest]] + spot[widest + 1:]
    return array.at[tuple(spot)].set(low).at[tuple(neighbour)].set(high)


def raised(drawn, own_key, source, target, parts, factor):
    def block_of(dim):
        return (jnp.arange(drawn.shape[dim]) // (drawn.shape[dim] // parts)).reshape((-1,) + (1,) * (drawn.ndim - 1 - dim))

    first = jax.random.permutation(own_key, parts)[block_of(target)]
    far = (block_of(target) + parts // 2) % parts
    return jnp.where((block_of(source) == first) | (block_of(source) == far), factor * drawn, drawn)


def level_of(key, extent, pieces, least, largest):
    loudness, own = 1.0, jax.random.fold_in(key, 6)
    for dim, parts in pieces:
        heights = jnp.exp(jax.random.uniform(jax.random.fold_in(own, dim), (parts,), jnp.float32, least / len(pieces), largest / len(pieces)))
        loudness = loudness * jnp.repeat(heights, extent[dim] // parts).reshape([-1 if axis == dim else 1 for axis in range(len(extent))])
    return loudness


def split_up(count, total, limit, lean):
    portions = [(1 << 20) // math.isqrt(standing ** lean) + 1 for standing in range(2, count + 1)]
    rest, given = total - limit - (count - 1), [1] * (count - 1)
    while rest > 0:
        free = [i for i in range(count - 1) if given[i] < limit]
        whole, budget = sum([portions[i] for i in free]), rest
        for i in free:
            extra = min(limit - given[i], max(1, budget * portions[i] // whole), rest)
            given[i] = given[i] + extra
            rest = rest - extra
    return np.array([limit] + given)


def ragged(own_key, count, total, reach, skew):
    if count == 2:
        one = jax.random.randint(own_key, (), max(1, total - reach), min(reach, total - 1) + 1)
        return jnp.stack([one, total - one])
    sizes = jnp.asarray(split_up(count, total, reach, skew), jnp.int32)
    twos = (count - 1) // 2
    source_of, taker = sizes[1:1 + 2 * twos:2], sizes[2:2 + 2 * twos:2]
    slack = jnp.minimum(source_of - 1, reach - taker)
    moved = jax.random.randint(jax.random.fold_in(own_key, 1), (twos,), 0, 1 << 20) % (slack + 1)
    sizes = sizes.at[1:1 + 2 * twos:2].set(source_of - moved).at[2:2 + 2 * twos:2].set(taker + moved)
    return sizes[jax.random.permutation(jax.random.fold_in(own_key, 2), count)]


def centred(rng, shape, width, limit, shards=(), held_as=jnp.bfloat16):
    values = width * jax.random.normal(rng, shape, jnp.float32)
    if shards:
        values = values * level_of(rng, shape, shards, -0.22, 0.18)
    return jnp.clip(values, -limit, limit).astype(held_as)


def noise_with(stream_key, extent, deviation, most, cuts, heavy, kind=jnp.bfloat16):
    values = deviation * jax.random.normal(stream_key, extent, jnp.float32)
    if cuts:
        values = values * level_of(stream_key, extent, cuts, -0.22, 0.18)
    return jnp.clip(raised(values, jax.random.fold_in(stream_key, 3), *heavy), -most, most).astype(kind)


def setup_inputs(seed: int = 0) -> dict:
    seeds = jax.random.split(jax.random.key(seed), 11)
    feats = centred(seeds[0], (VERTICES, F_IN), 1.0, 6.0, ((0, 256),))
    w_self = centred(seeds[1], (F_IN, F_OUT), F_IN ** -0.5, 0.5)
    w_neigh = centred(seeds[2], (F_IN, F_OUT), F_IN ** -0.5, 0.5)
    bias = centred(seeds[3], (F_OUT,), 0.1, 0.6, (), jnp.float32)
    cotangent = noise_with(seeds[4], (VERTICES, F_OUT), 1.0, 24.0, ((0, 256),), (0, 1, 256, 6.0))
    send_rows = place_ends(jax.random.randint(seeds[5], (N_VERT, N_VERT, C_REST), 0, V_DEV), jax.random.fold_in(seeds[5], 1), 0, V_DEV - 1).astype(jnp.int32)
    hub_ids = draw_hub_ids(jax.random.fold_in(seeds[10], 71), 0)
    edge_src = draw_edge_src(jax.random.fold_in(seeds[10], 71), 0)
    edge_dst = jax.vmap(lambda own: jnp.searchsorted(jnp.cumsum(ragged(own, V_DEV, E_DEV, DEG_MOST, 2)), jnp.arange(E_DEV), side="right"))(jax.random.split(seeds[8], N_VERT)).reshape((N_VERT, E_DEV)).astype(jnp.int32)
    edge_count = ragged(seeds[9], N_VERT, N_VERT * E_DEV * 2 // 5, E_DEV, 2).astype(jnp.int32)
    return dict(feats=feats, w_self=w_self, w_neigh=w_neigh, bias=bias, cotangent=cotangent, send_rows=send_rows, hub_ids=hub_ids, edge_src=edge_src, edge_dst=edge_dst, edge_count=edge_count)


def silu_slope(linear):
    logistic = jax.nn.sigmoid(linear)
    return logistic * (1.0 + linear * (1.0 - logistic))


def reference(feats, w_self, w_neigh, bias, cotangent, send_rows, hub_ids, edge_src, edge_dst, edge_count):
    owner_base = jnp.arange(N_VERT, dtype=jnp.int32) * V_DEV
    local_ids = jnp.arange(V_DEV, dtype=jnp.int32)
    edge_ids = jnp.arange(E_DEV, dtype=jnp.int32)
    table_rows = V_DEV + N_VERT * C_REST + HUBS

    def device_step(running, device):
        grad_feats, grad_w_self, grad_w_neigh, grad_bias = running
        block_start = device * V_DEV
        own_feats = lax.dynamic_slice_in_dim(feats, block_start, V_DEV, 0)
        upstream = lax.dynamic_slice_in_dim(cotangent, block_start, V_DEV, 0)
        send_plan = lax.dynamic_index_in_dim(send_rows, device, 1, keepdims=False)
        halo_ids = (owner_base[:, None] + send_plan).reshape(-1).astype(jnp.int32)
        table_ids = jnp.concatenate([(block_start + local_ids).astype(jnp.int32), halo_ids, hub_ids.astype(jnp.int32)])
        source_table = feats[table_ids]
        edge_from = lax.dynamic_index_in_dim(edge_src, device, 0, keepdims=False)
        edge_to = lax.dynamic_index_in_dim(edge_dst, device, 0, keepdims=False)
        real_count = lax.dynamic_index_in_dim(edge_count, device, 0, keepdims=False)
        is_real = edge_ids < real_count
        drop_to = jnp.where(is_real, edge_to, V_DEV)
        degree = jax.ops.segment_sum(is_real.astype(jnp.float32), drop_to, num_segments=V_DEV)
        inverse = 1.0 / jnp.maximum(degree, 1.0)
        summed = jax.ops.segment_sum(source_table[edge_from].astype(jnp.float32), drop_to, num_segments=V_DEV)
        mean_rows = (summed * inverse[:, None]).astype(jnp.bfloat16)
        linear = jnp.dot(own_feats, w_self, preferred_element_type=jnp.float32)
        linear = linear + jnp.dot(mean_rows, w_neigh, preferred_element_type=jnp.float32) + bias
        output = jax.nn.silu(linear).astype(jnp.bfloat16)
        grad_linear = (upstream.astype(jnp.float32) * silu_slope(linear)).astype(jnp.bfloat16)
        grad_w_self = grad_w_self + jnp.dot(own_feats.T, grad_linear, preferred_element_type=jnp.float32)
        grad_w_neigh = grad_w_neigh + jnp.dot(mean_rows.T, grad_linear, preferred_element_type=jnp.float32)
        grad_bias = grad_bias + jnp.sum(grad_linear.astype(jnp.float32), axis=0)
        own_grad = jnp.dot(grad_linear, w_self.T, preferred_element_type=jnp.float32)
        spread = jnp.dot(grad_linear, w_neigh.T, preferred_element_type=jnp.float32) * inverse[:, None]
        drop_from = jnp.where(is_real, edge_from, table_rows)
        back_table = jax.ops.segment_sum(spread[edge_to], drop_from, num_segments=table_rows)
        back_table = back_table.at[:V_DEV].add(own_grad)
        grad_feats = grad_feats.at[table_ids].add(back_table)
        return (grad_feats, grad_w_self, grad_w_neigh, grad_bias), output

    initial = (
        jnp.zeros((V_DEV * N_VERT, F_IN), jnp.float32),
        jnp.zeros((F_IN, F_OUT), jnp.float32),
        jnp.zeros((F_IN, F_OUT), jnp.float32),
        jnp.zeros((F_OUT,), jnp.float32),
    )
    running, blocks = lax.scan(device_step, initial, jnp.arange(N_VERT, dtype=jnp.int32))
    grad_feats, grad_w_self, grad_w_neigh, grad_bias = running
    output = blocks.reshape(V_DEV * N_VERT, F_OUT)
    return (output, grad_feats.astype(jnp.bfloat16), grad_w_self, grad_w_neigh, grad_bias)
```

```python
import functools

import jax
import jax.numpy as jnp
from jax import lax
from jax.experimental import pallas as pl
from jax.experimental.pallas import tpu as pltpu
from jax.sharding import PartitionSpec as P

HUB_MOST = 8
STREAMS = 8
UNROLL = 4
GROUP = STREAMS * UNROLL
LIMIT = 60 * 1024 * 1024
F32 = jnp.float32
BF16 = jnp.bfloat16
SMEM = pl.BlockSpec(memory_space=pltpu.SMEM)
VMEM = pl.BlockSpec(memory_space=pltpu.VMEM)


def up(n, k):
    return -(-n // k) * k


def row(i):
    return pl.ds(i, 1)


def clear(refs, rows, step):
    def some(i, _):
        at = pl.ds(pl.multiple_of(i * step, step), step)
        for ref in refs:
            ref[at, :] = jnp.zeros((step, ref.shape[1]), F32)
        return 0

    lax.fori_loop(0, rows // step, some, 0)


def add_rows(trips, take, put, table, sums):
    def some(i, _):
        for j in range(GROUP):
            e = i * GROUP + j
            to = row(put[e])
            ref = sums[j % STREAMS]
            ref[to, :] = ref[to, :] + table[row(take[e]), :]
        return 0

    lax.fori_loop(0, trips, some, 0)


def total(sums, at):
    parts = [ref[at, :] for ref in sums]
    while len(parts) > 1:
        parts = [a + b for a, b in zip(parts[::2], parts[1::2])]
    return parts[0]


def widen(ref, table, slots, first, start):
    blocks = 16

    def some(i, _):
        part = ref[pl.ds(i * blocks, blocks), first : first + slots, :]
        at = pl.multiple_of(start + i * blocks * slots, 8)
        table[pl.ds(at, blocks * slots), :] = part.astype(F32).reshape(blocks * slots, -1)
        return 0

    lax.fori_loop(0, ref.shape[0] // blocks, some, 0)


def gather_kernel(send_ref, hub_ref, feats_ref, out_ref, table, rows):
    peers, depth, width = out_ref.shape
    slots = depth - HUB_MOST
    table[...] = feats_ref[...].astype(F32)

    def some(i, _):
        for j in range(GROUP):
            e = i * GROUP + j
            rows[row(e), :] = table[row(send_ref[e]), :]
        return 0

    lax.fori_loop(0, peers * slots // GROUP, some, 0)
    hubs = jnp.concatenate([table[row(hub_ref[j]), :] for j in range(HUB_MOST)], axis=0)
    hubs = jnp.broadcast_to(hubs[None], (16, HUB_MOST, width)).astype(BF16)

    def pack(i, _):
        at = pl.multiple_of(i * 16 * slots, 8)
        own = rows[pl.ds(at, 16 * slots), :].reshape(16, slots, width).astype(BF16)
        out_ref[pl.ds(i * 16, 16), :slots, :] = own
        out_ref[pl.ds(i * 16, 16), slots:, :] = hubs
        return 0

    lax.fori_loop(0, peers // 16, pack, 0)


def layer_kernel(
    trips_ref, src_ref, dst_ref, place_ref,
    feats_ref, arrived_ref, inverse_ref, cot_ref, w_self_ref, w_neigh_ref, bias_ref,
    out_ref, own_ref, outgoing_ref, grads_ref,
    table, hub_slots, spread, *sums,
):
    local, width = feats_ref.shape
    peers, depth, _ = arrived_ref.shape
    slots = depth - HUB_MOST
    hubs = place_ref.shape[0]
    wide = w_self_ref.shape[1]
    halo_end = local + peers * slots
    trips = trips_ref[0]
    step = 256

    clear(sums, up(local + 1, 64), 64)
    table[:local, :] = feats_ref[...].astype(F32)
    widen(arrived_ref, table, slots, 0, local)
    widen(arrived_ref, hub_slots, HUB_MOST, slots, 0)

    def hub_in(i, _):
        for j in range(8):
            h = i * 8 + j
            table[row(halo_end + h), :] = hub_slots[row(place_ref[h]), :]
        return 0

    lax.fori_loop(0, hubs // 8, hub_in, 0)
    add_rows(trips, src_ref, dst_ref, table, sums)

    grads_ref[...] = jnp.zeros_like(grads_ref)
    w_self, w_neigh, bias = w_self_ref[...], w_neigh_ref[...], bias_ref[...]
    outer = (((0,), (0,)), ((), ()))
    back = (((1,), (1,)), ((), ()))

    def dense(i, _):
        at = pl.ds(pl.multiple_of(i * step, step), step)
        feats = feats_ref[at, :]
        inverse = inverse_ref[at, :]
        mean = (total(sums, at) * inverse).astype(BF16)
        linear = jnp.dot(feats, w_self, preferred_element_type=F32)
        linear = linear + jnp.dot(mean, w_neigh, preferred_element_type=F32) + bias
        logistic = jax.nn.sigmoid(linear)
        out_ref[at, :] = (linear * logistic).astype(BF16)
        slope = logistic * (1.0 + linear * (1.0 - logistic))
        grad = (cot_ref[at, :].astype(F32) * slope).astype(BF16)
        grads_ref[:width, :] += lax.dot_general(feats, grad, outer, preferred_element_type=F32)
        grads_ref[width : 2 * width, :] += lax.dot_general(
            mean, grad, outer, preferred_element_type=F32
        )
        grads_ref[2 * width : 2 * width + 8, :] += jnp.sum(
            grad.astype(F32).reshape(step // 8, 8, wide), axis=0
        )
        own_ref[at, :] = lax.dot_general(grad, w_self, back, preferred_element_type=F32)
        spread[at, :] = lax.dot_general(grad, w_neigh, back, preferred_element_type=F32) * inverse
        return 0

    lax.fori_loop(0, local // step, dense, 0)

    clear(sums, sums[0].shape[0], 64)
    spread[local : local + 8, :] = jnp.zeros((8, width), F32)
    add_rows(trips, dst_ref, src_ref, spread, sums)

    def own_part(i, _):
        at = pl.ds(pl.multiple_of(i * step, step), step)
        own_ref[at, :] += total(sums, at)
        return 0

    lax.fori_loop(0, local // step, own_part, 0)

    def halo_part(i, _):
        at = pl.ds(pl.multiple_of(local + i * 16 * slots, 8), 16 * slots)
        part = total(sums, at).reshape(16, slots, width).astype(BF16)
        outgoing_ref[pl.ds(i * 16, 16), :slots, :] = part
        return 0

    lax.fori_loop(0, peers // 16, halo_part, 0)

    clear((hub_slots,), peers * HUB_MOST, 64)

    def hub_part(i, _):
        at = pl.ds(pl.multiple_of(halo_end + i * 8, 8), 8)
        table[pl.ds(pl.multiple_of(i * 8, 8), 8), :] = total(sums, at)
        return 0

    lax.fori_loop(0, hubs // 8, hub_part, 0)

    def hub_out(i, _):
        for j in range(8):
            h = i * 8 + j
            hub_slots[row(place_ref[h]), :] = table[row(h), :]
        return 0

    lax.fori_loop(0, hubs // 8, hub_out, 0)

    def hub_pack(i, _):
        at = pl.ds(pl.multiple_of(i * 16 * HUB_MOST, 8), 16 * HUB_MOST)
        part = hub_slots[at, :].reshape(16, HUB_MOST, width).astype(BF16)
        outgoing_ref[pl.ds(i * 16, 16), slots:, :] = part
        return 0

    lax.fori_loop(0, peers // 16, hub_pack, 0)


def final_kernel(send_ref, hub_ref, own_ref, returned_ref, out_ref, rows, hub_sum, *sums):
    peers, depth, width = returned_ref.shape
    slots = depth - HUB_MOST
    local = own_ref.shape[0]
    step = 256
    sums[0][:local, :] = own_ref[...]
    clear(sums[1:], up(local + 1, 8) // 8 * 8, 8)
    widen(returned_ref, rows, slots, 0, 0)

    def some(i, _):
        for j in range(GROUP):
            e = i * GROUP + j
            to = row(send_ref[e])
            ref = sums[j % STREAMS]
            ref[to, :] = ref[to, :] + rows[row(e), :]
        return 0

    lax.fori_loop(0, peers * slots // GROUP, some, 0)

    def hub_add(i, acc):
        part = returned_ref[pl.ds(i * 16, 16), slots:, :].astype(F32)
        return acc + jnp.sum(part, axis=0)

    hub_sum[...] = lax.fori_loop(0, peers // 16, hub_add, jnp.zeros((HUB_MOST, width), F32))
    for j in range(HUB_MOST):
        to = row(hub_ref[j])
        sums[0][to, :] = sums[0][to, :] + hub_sum[row(j), :]

    def close(i, _):
        at = pl.ds(pl.multiple_of(i * step, step), step)
        out_ref[at, :] = total(sums, at).astype(BF16)
        return 0

    lax.fori_loop(0, local // step, close, 0)


def body(
    feats, w_self, w_neigh, bias, cotangent, send_rows, hub_ids, edge_src, edge_dst, edge_count
):
    local, width = feats.shape
    wide = w_self.shape[1]
    peers = lax.axis_size("vert")
    me = lax.axis_index("vert")
    slots = send_rows.shape[2]
    depth = slots + HUB_MOST
    hub_total = hub_ids.shape[0]
    table_rows = local + peers * slots + hub_total
    edge_total = edge_src.shape[1]
    params = pltpu.CompilerParams(vmem_limit_bytes=LIMIT)

    send = send_rows.reshape(-1)
    hub_owner = hub_ids // local
    hub_local = hub_ids - hub_owner * local
    order = lax.iota(jnp.int32, hub_total)
    first = jnp.sum((hub_owner < me).astype(jnp.int32))
    picked = (hub_owner == me)[None, :] & (
        (order - first)[None, :] == lax.iota(jnp.int32, HUB_MOST)[:, None]
    )
    own_count = jnp.sum((hub_owner == me).astype(jnp.int32))
    own_hubs = jnp.sum(jnp.where(picked, hub_local[None, :], 0), axis=1)
    own_back = jnp.where(lax.iota(jnp.int32, HUB_MOST) < own_count, own_hubs, local)
    before = jnp.sum((hub_owner[None, :] < hub_owner[:, None]).astype(jnp.int32), axis=1)
    place = hub_owner * HUB_MOST + order - before

    sent = pl.pallas_call(
        gather_kernel,
        out_shape=jax.ShapeDtypeStruct((peers, depth, width), BF16),
        in_specs=[SMEM, SMEM, VMEM],
        out_specs=VMEM,
        scratch_shapes=[
            pltpu.VMEM((local, width), F32),
            pltpu.VMEM((peers * slots, width), F32),
        ],
        compiler_params=params,
        name="gather_sent",
    )(send, own_hubs, feats)
    arrived = lax.all_to_all(sent, "vert", split_axis=0, concat_axis=0, tiled=True)

    is_real = lax.iota(jnp.int32, edge_total) < edge_count[0]
    dst = jnp.where(is_real, edge_dst[0], local)
    src = jnp.where(is_real, edge_src[0], table_rows)
    trips = (edge_count + (GROUP - 1)) // GROUP
    lanes = 128
    high = (dst // lanes)[:, None] == lax.iota(jnp.int32, local // lanes)[None, :]
    low = (dst % lanes)[:, None] == lax.iota(jnp.int32, lanes)[None, :]
    degree = lax.dot_general(
        high.astype(BF16), low.astype(BF16), (((0,), (0,)), ((), ())), preferred_element_type=F32
    ).reshape(-1)
    inverse = jnp.broadcast_to((1.0 / jnp.maximum(degree, 1.0))[:, None], (local, width))

    rows_up = up(table_rows + 1, 64)
    output, own, outgoing, grads = pl.pallas_call(
        layer_kernel,
        out_shape=(
            jax.ShapeDtypeStruct((local, wide), BF16),
            jax.ShapeDtypeStruct((local, width), F32),
            jax.ShapeDtypeStruct((peers, depth, width), BF16),
            jax.ShapeDtypeStruct((2 * width + 8, wide), F32),
        ),
        in_specs=[SMEM] * 4 + [VMEM] * 7,
        out_specs=(VMEM,) * 4,
        scratch_shapes=[
            pltpu.VMEM((rows_up, width), F32),
            pltpu.VMEM((peers * HUB_MOST, width), F32),
            pltpu.VMEM((up(local + 1, 8), width), F32),
        ]
        + [pltpu.VMEM((rows_up, width), F32)] * STREAMS,
        compiler_params=params,
        name="layer",
    )(trips, src, dst, place, feats, arrived, inverse, cotangent, w_self, w_neigh, bias[None, :])

    summed = lax.psum(grads, "vert")
    returned = lax.all_to_all(outgoing, "vert", split_axis=0, concat_axis=0, tiled=True)
    grad_feats = pl.pallas_call(
        final_kernel,
        out_shape=jax.ShapeDtypeStruct((local, width), BF16),
        in_specs=[SMEM, SMEM, VMEM, VMEM],
        out_specs=VMEM,
        scratch_shapes=[
            pltpu.VMEM((peers * slots, width), F32),
            pltpu.VMEM((HUB_MOST, width), F32),
        ]
        + [pltpu.VMEM((up(local + 1, 8), width), F32)] * STREAMS,
        compiler_params=params,
        name="final",
    )(send, own_back, own, returned)
    grad_bias = jnp.sum(summed[2 * width :], axis=0)
    return (output, grad_feats, summed[:width], summed[width : 2 * width], grad_bias)


def solution(mesh):
    in_specs = (
        P("vert", None),
        P(),
        P(),
        P(),
        P("vert", None),
        P("vert", None, None),
        P(),
        P("vert", None),
        P("vert", None),
        P("vert"),
    )
    out_specs = (P("vert", None), P("vert", None), P(), P(), P())
    return jax.shard_map(body, mesh=mesh, in_specs=in_specs, out_specs=out_specs, check_vma=False)
```

```python
import functools

import jax
import jax.numpy as jnp
from jax import lax
from jax.experimental import pallas as pl
from jax.experimental.pallas import tpu as pltpu
from jax.sharding import PartitionSpec as P

HUB_MOST = 8
STREAMS = 8
UNROLL = 4
GROUP = STREAMS * UNROLL
LIMIT = 60 * 1024 * 1024
F32 = jnp.float32
BF16 = jnp.bfloat16
SMEM = pl.BlockSpec(memory_space=pltpu.SMEM)
VMEM = pl.BlockSpec(memory_space=pltpu.VMEM)


def up(n, k):
    return -(-n // k) * k


def row(i):
    return pl.ds(i, 1)


def clear(refs, rows, step):
    def some(i, _):
        at = pl.ds(pl.multiple_of(i * step, step), step)
        for ref in refs:
            ref[at, :] = jnp.zeros((step, ref.shape[1]), F32)
        return 0

    lax.fori_loop(0, rows // step, some, 0)


def add_rows(trips, take, put, table, sums):
    def some(i, _):
        for j in range(GROUP):
            e = i * GROUP + j
            to = row(put[e])
            ref = sums[j % STREAMS]
            ref[to, :] = ref[to, :] + table[row(take[e]), :]
        return 0

    lax.fori_loop(0, trips, some, 0)


def total(sums, at):
    parts = [ref[at, :] for ref in sums]
    while len(parts) > 1:
        parts = [a + b for a, b in zip(parts[::2], parts[1::2])]
    return parts[0]


def widen(ref, table, start):
    blocks, slots = 16, ref.shape[1]

    def some(i, _):
        part = ref[pl.ds(i * blocks, blocks)]
        at = pl.multiple_of(start + i * blocks * slots, 8)
        table[pl.ds(at, blocks * slots), :] = part.astype(F32).reshape(blocks * slots, -1)
        return 0

    lax.fori_loop(0, ref.shape[0] // blocks, some, 0)


def gather_kernel(send_ref, hub_ref, feats_ref, out_ref, hub_out_ref, table, rows):
    peers, slots, width = out_ref.shape
    table[...] = feats_ref[...].astype(F32)

    def some(i, _):
        for j in range(GROUP):
            e = i * GROUP + j
            rows[row(e), :] = table[row(send_ref[e]), :]
        return 0

    lax.fori_loop(0, peers * slots // GROUP, some, 0)
    hubs = jnp.concatenate([table[row(hub_ref[j]), :] for j in range(HUB_MOST)], axis=0)
    hub_out_ref[...] = hubs.astype(BF16)

    def pack(i, _):
        at = pl.multiple_of(i * 16 * slots, 8)
        own = rows[pl.ds(at, 16 * slots), :].reshape(16, slots, width).astype(BF16)
        out_ref[pl.ds(i * 16, 16)] = own
        return 0

    lax.fori_loop(0, peers // 16, pack, 0)


def layer_kernel(
    trips_ref, src_ref, dst_ref, place_ref,
    feats_ref, halo_ref, hubs_ref, inverse_ref, cot_ref, w_self_ref, w_neigh_ref, bias_ref,
    out_ref, own_ref, halo_back_ref, hub_back_ref, grads_ref,
    table, hub_slots, spread, *sums,
):
    local, width = feats_ref.shape
    peers, slots, _ = halo_ref.shape
    hubs = place_ref.shape[0]
    wide = w_self_ref.shape[1]
    halo_end = local + peers * slots
    trips = trips_ref[0]
    step = 256

    clear(sums, up(local + 1, 64), 64)
    table[:local, :] = feats_ref[...].astype(F32)
    widen(halo_ref, table, local)
    widen(hubs_ref, hub_slots, 0)

    def hub_in(i, _):
        for j in range(8):
            h = i * 8 + j
            table[row(halo_end + h), :] = hub_slots[row(place_ref[h]), :]
        return 0

    lax.fori_loop(0, hubs // 8, hub_in, 0)
    add_rows(trips, src_ref, dst_ref, table, sums)

    grads_ref[...] = jnp.zeros_like(grads_ref)
    w_self, w_neigh, bias = w_self_ref[...], w_neigh_ref[...], bias_ref[...]
    outer = (((0,), (0,)), ((), ()))
    back = (((1,), (1,)), ((), ()))

    def dense(i, _):
        at = pl.ds(pl.multiple_of(i * step, step), step)
        feats = feats_ref[at, :]
        inverse = inverse_ref[at, :]
        mean = (total(sums, at) * inverse).astype(BF16)
        linear = jnp.dot(feats, w_self, preferred_element_type=F32)
        linear = linear + jnp.dot(mean, w_neigh, preferred_element_type=F32) + bias
        logistic = jax.nn.sigmoid(linear)
        out_ref[at, :] = (linear * logistic).astype(BF16)
        slope = logistic * (1.0 + linear * (1.0 - logistic))
        grad = (cot_ref[at, :].astype(F32) * slope).astype(BF16)
        grads_ref[:width, :wide] += lax.dot_general(feats, grad, outer, preferred_element_type=F32)
        grads_ref[width : 2 * width, :wide] += lax.dot_general(
            mean, grad, outer, preferred_element_type=F32
        )
        grad_sum = jnp.sum(grad.astype(F32).reshape(step // 8, 8, wide), axis=0)
        for j in range(wide // width):
            grads_ref[8 * j : 8 * j + 8, wide:] += grad_sum[:, j * width : (j + 1) * width]
        own_ref[at, :] = lax.dot_general(grad, w_self, back, preferred_element_type=F32)
        spread[at, :] = lax.dot_general(grad, w_neigh, back, preferred_element_type=F32) * inverse
        return 0

    lax.fori_loop(0, local // step, dense, 0)

    clear(sums, sums[0].shape[0], 64)
    spread[local : local + 8, :] = jnp.zeros((8, width), F32)
    add_rows(trips, dst_ref, src_ref, spread, sums)

    def own_part(i, _):
        at = pl.ds(pl.multiple_of(i * step, step), step)
        own_ref[at, :] += total(sums, at)
        return 0

    lax.fori_loop(0, local // step, own_part, 0)

    def halo_part(i, _):
        at = pl.ds(pl.multiple_of(local + i * 16 * slots, 8), 16 * slots)
        part = total(sums, at).reshape(16, slots, width).astype(BF16)
        halo_back_ref[pl.ds(i * 16, 16)] = part
        return 0

    lax.fori_loop(0, peers // 16, halo_part, 0)

    clear((hub_slots,), peers * HUB_MOST, 64)

    def hub_part(i, _):
        at = pl.ds(pl.multiple_of(halo_end + i * 8, 8), 8)
        table[pl.ds(pl.multiple_of(i * 8, 8), 8), :] = total(sums, at)
        return 0

    lax.fori_loop(0, hubs // 8, hub_part, 0)

    def hub_out(i, _):
        for j in range(8):
            h = i * 8 + j
            hub_slots[row(place_ref[h]), :] = table[row(h), :]
        return 0

    lax.fori_loop(0, hubs // 8, hub_out, 0)

    def hub_pack(i, _):
        at = pl.ds(pl.multiple_of(i * 16 * HUB_MOST, 8), 16 * HUB_MOST)
        part = hub_slots[at, :].reshape(16, HUB_MOST, width).astype(BF16)
        hub_back_ref[pl.ds(i * 16, 16)] = part
        return 0

    lax.fori_loop(0, peers // 16, hub_pack, 0)


def final_kernel(send_ref, hub_ref, own_ref, returned_ref, hub_sum, out_ref, rows, *sums):
    peers, slots, width = returned_ref.shape
    local = own_ref.shape[0]
    step = 256
    sums[0][:local, :] = own_ref[...]
    clear(sums[1:], up(local + 1, 8), 8)
    widen(returned_ref, rows, 0)

    def some(i, _):
        for j in range(GROUP):
            e = i * GROUP + j
            to = row(send_ref[e])
            ref = sums[j % STREAMS]
            ref[to, :] = ref[to, :] + rows[row(e), :]
        return 0

    lax.fori_loop(0, peers * slots // GROUP, some, 0)

    for j in range(HUB_MOST):
        to = row(hub_ref[j])
        sums[0][to, :] = sums[0][to, :] + hub_sum[row(j), :]

    def close(i, _):
        at = pl.ds(pl.multiple_of(i * step, step), step)
        out_ref[at, :] = total(sums, at).astype(BF16)
        return 0

    lax.fori_loop(0, local // step, close, 0)


PLANE = 32
MESH = pl.DeviceIdType.MESH


class Places:
    def __init__(self):
        self.count = lax.axis_size("vert")
        self.planes = self.count // PLANE
        self.me = lax.axis_index("vert")
        self.z = lax.div(self.me, PLANE)
        self.p = lax.rem(self.me, PLANE)

    def in_plane(self, i):
        p = lax.rem(self.p + i, PLANE)
        return p, self.z * PLANE + p

    def in_line(self, i):
        z = lax.rem(self.z + i, self.planes)
        return z, z * PLANE + self.p

    def barrier(self, ready):
        entry = pltpu.get_barrier_semaphore()

        def greet_plane(i, _):
            pl.semaphore_signal(entry, device_id=(self.in_plane(i)[1],), device_id_type=MESH)
            return 0

        def greet_line(i, _):
            pl.semaphore_signal(entry, device_id=(self.in_line(i)[1],), device_id_type=MESH)
            return 0

        def vouch(i, _):
            pl.semaphore_signal(ready, device_id=(self.in_line(i)[1],), device_id_type=MESH)
            return 0

        lax.fori_loop(1, PLANE, greet_plane, 0)
        lax.fori_loop(1, self.planes, greet_line, 0)
        pl.semaphore_wait(entry, PLANE + self.planes - 2)
        lax.fori_loop(1, self.planes, vouch, 0)
        pl.semaphore_wait(ready, self.planes - 1)

    def copy(self, src, dst, sems, to):
        return pltpu.make_async_remote_copy(
            src_ref=src,
            dst_ref=dst,
            send_sem=sems.at[0],
            recv_sem=sems.at[1],
            device_id=(to,),
            device_id_type=MESH,
        )

    def all_of(self, ref, sems):
        return self.copy(ref, ref, sems, lax.rem(self.me + 1, self.count))

    def send_blocks(self, src, dst, sems, start, stop):
        def some(k, _):
            t = lax.rem(self.me * 75 + k * 159, self.count)

            @pl.when(t != self.me)
            def _():
                self.copy(src.at[t], dst.at[self.me], sems, t).start()

            return 0

        lax.fori_loop(start, stop, some, 0)


def forward_kernel(sent_ref, hub_ref, halo_ref, hubs_ref, a, b, c, keep, ready):
    here = Places()
    here.barrier(ready)
    own_hub = pltpu.make_async_copy(hub_ref, hubs_ref.at[here.p, here.z], keep.at[0])
    own_hub.start()
    own_halo = pltpu.make_async_copy(sent_ref.at[here.me], halo_ref.at[here.me], keep.at[1])
    own_halo.start()

    def along(i, _):
        here.copy(hub_ref, hubs_ref.at[here.p, here.z], a, here.in_line(i)[1]).start()
        return 0

    lax.fori_loop(1, here.planes, along, 0)
    here.send_blocks(sent_ref, halo_ref, b, 0, here.count // 2)
    own_hub.wait()
    here.all_of(hubs_ref.at[here.p, pl.ds(0, here.planes - 1)], a).wait()

    def across(i, _):
        here.copy(hubs_ref.at[here.p], hubs_ref.at[here.p], c, here.in_plane(i)[1]).start()
        return 0

    lax.fori_loop(1, PLANE, across, 0)
    here.send_blocks(sent_ref, halo_ref, b, here.count // 2, here.count)
    own_halo.wait()
    here.all_of(hubs_ref.at[pl.ds(0, PLANE - 1)], c).wait()
    here.all_of(halo_ref.at[pl.ds(0, here.count - 1)], b).wait()


def backward_kernel(
    back_ref, hub_ref, grads_ref, halo_ref, hub_sum_ref, whole_ref,
    part_in, hub_in, grads_in, hub_part, hub_line, grad_part, grad_line,
    a, b, c, d, e, f, keep, ready,
):
    here = Places()
    part_in[...] = grads_ref[...].astype(BF16)
    here.barrier(ready)
    kept = [
        pltpu.make_async_copy(back_ref.at[here.me], halo_ref.at[here.me], keep.at[0]),
        pltpu.make_async_copy(hub_ref.at[here.p], hub_in.at[here.p], keep.at[1]),
        pltpu.make_async_copy(part_in.at[here.p], grads_in.at[here.p], keep.at[2]),
    ]
    for copy in kept:
        copy.start()

    def across(i, _):
        p, to = here.in_plane(i)
        here.copy(part_in.at[p], grads_in.at[here.p], a, to).start()
        here.copy(hub_ref.at[p], hub_in.at[here.p], b, to).start()
        return 0

    lax.fori_loop(1, PLANE, across, 0)
    third = here.count // 3
    here.send_blocks(back_ref, halo_ref, c, 0, third)
    for copy in kept:
        copy.wait()
    here.all_of(grads_in.at[pl.ds(0, PLANE - 1)], a).wait()
    here.all_of(hub_in.at[pl.ds(0, PLANE - 1)], b).wait()
    grad_part[...] = lax.fori_loop(
        0, PLANE, lambda i, acc: acc + grads_in[i].astype(F32), jnp.zeros(grad_part.shape, F32)
    )
    hub_part[...] = lax.fori_loop(
        0, PLANE, lambda i, acc: acc + hub_in[i].astype(F32), jnp.zeros(hub_part.shape, F32)
    )
    here.send_blocks(back_ref, halo_ref, c, third, third + 8)
    kept = [
        pltpu.make_async_copy(grad_part, grad_line.at[here.z], keep.at[0]),
        pltpu.make_async_copy(hub_part.at[here.z], hub_line.at[here.z], keep.at[1]),
    ]
    for copy in kept:
        copy.start()

    def along(i, _):
        z, to = here.in_line(i)
        here.copy(grad_part, grad_line.at[here.z], d, to).start()
        here.copy(hub_part.at[z], hub_line.at[here.z], e, to).start()
        return 0

    lax.fori_loop(1, here.planes, along, 0)
    here.send_blocks(back_ref, halo_ref, c, third + 8, 2 * third)
    for copy in kept:
        copy.wait()
    here.all_of(grad_line.at[pl.ds(0, here.planes - 1)], d).wait()
    here.all_of(hub_line.at[pl.ds(0, here.planes - 1)], e).wait()
    whole = grad_line[0]
    hub_sum = hub_line[0]
    for i in range(1, here.planes):
        whole = whole + grad_line[i]
        hub_sum = hub_sum + hub_line[i]
    grad_part[...] = whole
    hub_sum_ref[...] = hub_sum
    here.send_blocks(back_ref, halo_ref, c, 2 * third, 2 * third + 8)
    kept = pltpu.make_async_copy(grad_part, whole_ref.at[here.p], keep.at[0])
    kept.start()

    def spread(i, _):
        here.copy(grad_part, whole_ref.at[here.p], f, here.in_plane(i)[1]).start()
        return 0

    lax.fori_loop(1, PLANE, spread, 0)
    here.send_blocks(back_ref, halo_ref, c, 2 * third + 8, here.count)
    kept.wait()
    here.all_of(whole_ref.at[pl.ds(0, PLANE - 1)], f).wait()
    here.all_of(halo_ref.at[pl.ds(0, here.count - 1)], c).wait()


def body(
    feats, w_self, w_neigh, bias, cotangent, send_rows, hub_ids, edge_src, edge_dst, edge_count
):
    local, width = feats.shape
    wide = w_self.shape[1]
    peers = lax.axis_size("vert")
    me = lax.axis_index("vert")
    slots = send_rows.shape[2]
    hub_total = hub_ids.shape[0]
    table_rows = local + peers * slots + hub_total
    edge_total = edge_src.shape[1]
    params = pltpu.CompilerParams(vmem_limit_bytes=LIMIT)

    send = send_rows.reshape(-1)
    hub_owner = hub_ids // local
    hub_local = hub_ids - hub_owner * local
    order = lax.iota(jnp.int32, hub_total)
    first = jnp.sum((hub_owner < me).astype(jnp.int32))
    picked = (hub_owner == me)[None, :] & (
        (order - first)[None, :] == lax.iota(jnp.int32, HUB_MOST)[:, None]
    )
    own_count = jnp.sum((hub_owner == me).astype(jnp.int32))
    own_hubs = jnp.sum(jnp.where(picked, hub_local[None, :], 0), axis=1)
    own_back = jnp.where(lax.iota(jnp.int32, HUB_MOST) < own_count, own_hubs, local)
    before = jnp.sum((hub_owner[None, :] < hub_owner[:, None]).astype(jnp.int32), axis=1)
    planes = peers // PLANE
    block = (hub_owner % PLANE) * planes + hub_owner // PLANE
    place = block * HUB_MOST + order - before

    sent, own_rows = pl.pallas_call(
        gather_kernel,
        out_shape=(
            jax.ShapeDtypeStruct((peers, slots, width), BF16),
            jax.ShapeDtypeStruct((HUB_MOST, width), BF16),
        ),
        in_specs=[SMEM, SMEM, VMEM],
        out_specs=(VMEM, VMEM),
        scratch_shapes=[
            pltpu.VMEM((local, width), F32),
            pltpu.VMEM((peers * slots, width), F32),
        ],
        compiler_params=params,
        name="gather_sent",
    )(send, own_hubs, feats)
    pair = pltpu.SemaphoreType.DMA((2,))
    halo, hubs = pl.pallas_call(
        forward_kernel,
        out_shape=(
            jax.ShapeDtypeStruct((peers, slots, width), BF16),
            jax.ShapeDtypeStruct((PLANE, planes, HUB_MOST, width), BF16),
        ),
        in_specs=[VMEM, VMEM],
        out_specs=(VMEM, VMEM),
        scratch_shapes=[pair] * 4 + [pltpu.SemaphoreType.REGULAR],
        compiler_params=pltpu.CompilerParams(
            vmem_limit_bytes=LIMIT, collective_id=0, has_side_effects=True
        ),
        name="forward_exchange",
    )(sent, own_rows)
    hubs = hubs.reshape(peers, HUB_MOST, width)

    is_real = lax.iota(jnp.int32, edge_total) < edge_count[0]
    dst = jnp.where(is_real, edge_dst[0], local)
    src = jnp.where(is_real, edge_src[0], table_rows)
    trips = (edge_count + (GROUP - 1)) // GROUP
    lanes = 128
    high = (dst // lanes)[:, None] == lax.iota(jnp.int32, local // lanes)[None, :]
    low = (dst % lanes)[:, None] == lax.iota(jnp.int32, lanes)[None, :]
    degree = lax.dot_general(
        high.astype(BF16), low.astype(BF16), (((0,), (0,)), ((), ())), preferred_element_type=F32
    ).reshape(-1)
    inverse = jnp.broadcast_to((1.0 / jnp.maximum(degree, 1.0))[:, None], (local, width))

    rows_up = up(table_rows + 1, 64)
    output, own, halo_back, hub_back, grads = pl.pallas_call(
        layer_kernel,
        out_shape=(
            jax.ShapeDtypeStruct((local, wide), BF16),
            jax.ShapeDtypeStruct((local, width), F32),
            jax.ShapeDtypeStruct((peers, slots, width), BF16),
            jax.ShapeDtypeStruct((peers, HUB_MOST, width), BF16),
            jax.ShapeDtypeStruct((2 * width, wide + width), F32),
        ),
        in_specs=[SMEM] * 4 + [VMEM] * 8,
        out_specs=(VMEM,) * 5,
        scratch_shapes=[
            pltpu.VMEM((rows_up, width), F32),
            pltpu.VMEM((peers * HUB_MOST, width), F32),
            pltpu.VMEM((up(local + 1, 8), width), F32),
        ]
        + [pltpu.VMEM((rows_up, width), F32)] * STREAMS,
        compiler_params=params,
        name="layer",
    )(trips, src, dst, place, feats, halo, hubs, inverse, cotangent, w_self, w_neigh, bias[None, :])

    piece = (2 * width // PLANE, wide + width)
    returned, hub_sum, whole = pl.pallas_call(
        backward_kernel,
        out_shape=(
            jax.ShapeDtypeStruct((peers, slots, width), BF16),
            jax.ShapeDtypeStruct((HUB_MOST, width), F32),
            jax.ShapeDtypeStruct((PLANE,) + piece, F32),
        ),
        in_specs=[VMEM] * 3,
        out_specs=(VMEM,) * 3,
        scratch_shapes=[
            pltpu.VMEM((PLANE,) + piece, BF16),
            pltpu.VMEM((PLANE, planes, HUB_MOST, width), BF16),
            pltpu.VMEM((PLANE,) + piece, BF16),
            pltpu.VMEM((planes, HUB_MOST, width), F32),
            pltpu.VMEM((planes, HUB_MOST, width), F32),
            pltpu.VMEM(piece, F32),
            pltpu.VMEM((planes,) + piece, F32),
        ]
        + [pair] * 6
        + [pltpu.SemaphoreType.DMA((3,)), pltpu.SemaphoreType.REGULAR],
        compiler_params=pltpu.CompilerParams(
            vmem_limit_bytes=LIMIT, collective_id=1, has_side_effects=True
        ),
        name="backward_exchange",
    )(
        halo_back,
        hub_back.reshape(PLANE, planes, HUB_MOST, width),
        grads.reshape((PLANE,) + piece),
    )
    whole = whole.reshape(2 * width, wide + width)
    grad_feats = pl.pallas_call(
        final_kernel,
        out_shape=jax.ShapeDtypeStruct((local, width), BF16),
        in_specs=[SMEM, SMEM, VMEM, VMEM, VMEM],
        out_specs=VMEM,
        scratch_shapes=[
            pltpu.VMEM((peers * slots, width), F32),
        ]
        + [pltpu.VMEM((up(local + 1, 8), width), F32)] * STREAMS,
        compiler_params=params,
        name="final",
    )(send, own_back, own, returned, hub_sum)
    grad_bias = jnp.concatenate(
        [jnp.sum(whole[8 * j : 8 * j + 8, wide:], axis=0) for j in range(wide // width)]
    )
    return (output, grad_feats, whole[:width, :wide], whole[width:, :wide], grad_bias)


def solution(mesh):
    in_specs = (
        P("vert", None),
        P(),
        P(),
        P(),
        P("vert", None),
        P("vert", None, None),
        P(),
        P("vert", None),
        P("vert", None),
        P("vert"),
    )
    out_specs = (P("vert", None), P("vert", None), P(), P(), P())
    return jax.shard_map(body, mesh=mesh, in_specs=in_specs, out_specs=out_specs, check_vma=False)
```

```python
import functools

import jax
import jax.numpy as jnp
from jax import lax
from jax.experimental import pallas as pl
from jax.experimental.pallas import tpu as pltpu
from jax.sharding import PartitionSpec as P

HUB_MOST = 8
STREAMS = 8
GROUP = 32
CHUNK = 256
WINDOW = 64
LIMIT = 60 * 1024 * 1024
F32 = jnp.float32
BF16 = jnp.bfloat16
SMEM = pl.BlockSpec(memory_space=pltpu.SMEM)
VMEM = pl.BlockSpec(memory_space=pltpu.VMEM)


def up(n, k):
    return -(-n // k) * k


def row(i):
    return pl.ds(i, 1)


def tile(i, step):
    return pl.ds(pl.multiple_of(i * step, step), step)


def clear(refs, rows, step):
    def some(i, _):
        for ref in refs:
            ref[tile(i, step), :] = jnp.zeros((step, ref.shape[1]), F32)
        return 0

    lax.fori_loop(0, rows // step, some, 0)


def total(sums, at):
    parts = [ref[at, :] for ref in sums]
    while len(parts) > 1:
        parts = [a + b for a, b in zip(parts[::2], parts[1::2])]
    return parts[0]


def widen(ref, table, start):
    blocks, slots = 16, ref.shape[1]

    def some(i, _):
        part = ref[pl.ds(i * blocks, blocks)]
        at = pl.multiple_of(start + i * blocks * slots, 8)
        table[pl.ds(at, blocks * slots), :] = part.astype(F32).reshape(blocks * slots, -1)
        return 0

    lax.fori_loop(0, ref.shape[0] // blocks, some, 0)


def each_hub(hub_ref, local, planes, visit):
    shift = local.bit_length() - 1

    def some(i, carry):
        last, offset = carry
        for j in range(8):
            h = i * 8 + j
            owner = hub_ref[h] >> shift
            offset = jnp.where(owner == last, offset + 1, 0)
            block = lax.rem(owner, PLANE) * planes + lax.div(owner, PLANE)
            visit(h, block * HUB_MOST + offset)
            last = owner
        return last, offset

    lax.fori_loop(0, hub_ref.shape[0] // 8, some, (jnp.int32(-1), jnp.int32(0)))


def gather_kernel(hub_ref, send_ref, feats_ref, out_ref, hub_out_ref, back_ref, table, rows):
    peers, slots, width = out_ref.shape
    local = feats_ref.shape[0]
    hubs = hub_ref.shape[0]
    table[...] = feats_ref[...].astype(F32)

    def some(i, _):
        for j in range(GROUP):
            p, c = i * (GROUP // slots) + j // slots, j % slots
            rows[row(i * GROUP + j), :] = table[row(send_ref[c, p]), :]
        return 0

    lax.fori_loop(0, peers * slots // GROUP, some, 0)
    start = lax.axis_index("vert") * local

    def look(i, carry):
        first, after = carry
        for j in range(8):
            at = hub_ref[i * 8 + j] - start
            first = first + (at < 0).astype(jnp.int32)
            after = after + (at < local).astype(jnp.int32)
        return first, after

    first, after = lax.fori_loop(0, hubs // 8, look, (jnp.int32(0), jnp.int32(0)))
    own = []
    for j in range(HUB_MOST):
        here = jnp.minimum(first + j, jnp.maximum(after - 1, 0))
        at = jnp.clip(hub_ref[here] - start, 0, local - 1)
        own.append(table[row(at), :])
        back_ref[j] = jnp.where(first + j < after, at, local)
    hub_out_ref[...] = jnp.concatenate(own, axis=0).astype(BF16)

    def pack(i, _):
        part = rows[tile(i, 16 * slots), :].reshape(16, slots, width).astype(BF16)
        out_ref[pl.ds(i * 16, 16)] = part
        return 0

    lax.fori_loop(0, peers // 16, pack, 0)


def one_hot(lanes_ref, c, base, count):
    halves = []
    for h in range(CHUNK // 128):
        r = c * (CHUNK // 128) + h
        ends = lanes_ref[row(r), :] - base
        e = r * 128 + lax.broadcasted_iota(jnp.int32, (1, 128), 1)
        ends = jnp.where(e < count, ends, -1)
        hit = lax.broadcasted_iota(jnp.int32, (WINDOW, 128), 0) == ends
        halves.append(jnp.where(hit, 1.0, 0.0).astype(BF16))
    return jnp.concatenate(halves, axis=1)


def layer_kernel(
    count_ref, src_ref, dst_ref, hub_ref,
    lanes_ref, feats_ref, halo_ref, hubs_ref, cot_ref, w_self_ref, w_neigh_ref, bias_ref,
    out_ref, own_ref, halo_back_ref, hub_back_ref, grads_ref,
    table, hub_slots, spread, summed, degrees, even, odd, *sums,
):
    local, width = feats_ref.shape
    peers, slots, _ = halo_ref.shape
    hubs = hub_ref.shape[0]
    wide = w_self_ref.shape[1]
    halo_end = local + peers * slots
    last_chunk = src_ref.shape[0] // CHUNK - 1
    count = count_ref[0]
    pairs = lax.div(count + (2 * CHUNK - 1), 2 * CHUNK)
    step = 256
    outer = (((0,), (0,)), ((), ()))
    back = (((1,), (1,)), ((), ()))

    def base_of(c):
        return lax.shift_left(lax.shift_right_logical(dst_ref[c * CHUNK], 3), 3)

    def windows_of(c):
        return lax.div(dst_ref[c * CHUNK + CHUNK - 1] - base_of(c), WINDOW) + 1

    clear((summed, degrees), summed.shape[0], WINDOW)
    table[:local, :] = feats_ref[...].astype(F32)
    widen(halo_ref, table, local)
    widen(hubs_ref, hub_slots, 0)

    def hub_in(h, slot):
        table[row(halo_end + h), :] = hub_slots[row(slot), :]

    each_hub(hub_ref, local, peers // PLANE, hub_in)

    def fetch(c, rows):
        for j in range(CHUNK):
            rows[j : j + 1, :] = table[row(src_ref[c * CHUNK + j]), :]

    def reduce(c, rows, k):
        base = pl.multiple_of(base_of(c) + k * WINDOW, 8)
        at = pl.ds(base, WINDOW)
        right = jnp.concatenate([rows[...].astype(BF16), jnp.ones((CHUNK, width), BF16)], axis=1)
        part = jnp.dot(one_hot(lanes_ref, c, base, count), right, preferred_element_type=F32)
        summed[at, :] += part[:, :width]
        degrees[at, :] += part[:, width:]

    def reduce_more(c, rows):
        def some(k, _):
            reduce(c, rows, k)
            return 0

        lax.fori_loop(1, windows_of(c), some, 0)

    fetch(0, even)

    def forward(i, _):
        c = 2 * i
        reduce(c, even, 0)
        fetch(c + 1, odd)
        reduce_more(c, even)
        reduce(c + 1, odd, 0)
        fetch(jnp.minimum(c + 2, last_chunk), even)
        reduce_more(c + 1, odd)
        return 0

    lax.fori_loop(0, pairs, forward, 0)

    grads_ref[...] = jnp.zeros_like(grads_ref)
    w_self, w_neigh, bias = w_self_ref[...], w_neigh_ref[...], bias_ref[...]

    def dense(i, _):
        at = tile(i, step)
        feats = feats_ref[at, :]
        inverse = 1.0 / jnp.maximum(degrees[at, :], 1.0)
        mean = (summed[at, :] * inverse).astype(BF16)
        linear = jnp.dot(feats, w_self, preferred_element_type=F32)
        linear = linear + jnp.dot(mean, w_neigh, preferred_element_type=F32) + bias
        logistic = jax.nn.sigmoid(linear)
        out_ref[at, :] = (linear * logistic).astype(BF16)
        slope = logistic * (1.0 + linear * (1.0 - logistic))
        grad = (cot_ref[at, :].astype(F32) * slope).astype(BF16)
        grads_ref[:width, :wide] += lax.dot_general(feats, grad, outer, preferred_element_type=F32)
        grads_ref[width : 2 * width, :wide] += lax.dot_general(
            mean, grad, outer, preferred_element_type=F32
        )
        grad_sum = jnp.sum(grad.astype(F32).reshape(step // 8, 8, wide), axis=0)
        for j in range(wide // width):
            grads_ref[8 * j : 8 * j + 8, wide:] += grad_sum[:, j * width : (j + 1) * width]
        own_ref[at, :] = lax.dot_general(grad, w_self, back, preferred_element_type=F32)
        spread[at, :] = lax.dot_general(grad, w_neigh, back, preferred_element_type=F32) * inverse
        return 0

    lax.fori_loop(0, local // step, dense, 0)

    clear(sums, sums[0].shape[0], 64)
    spread[local:, :] = jnp.zeros((spread.shape[0] - local, width), F32)

    def expand(c, k):
        base = pl.multiple_of(base_of(c) + k * WINDOW, 8)
        values = spread[pl.ds(base, WINDOW), :]
        high = values.astype(BF16)
        low = (values - high.astype(F32)).astype(BF16)
        both = lax.dot_general(
            one_hot(lanes_ref, c, base, count),
            jnp.concatenate([high, low], axis=1),
            outer,
            preferred_element_type=F32,
        )
        return both[:, :width] + both[:, width:]

    def expand_more(c, rows):
        def some(k, _):
            rows[...] += expand(c, k)
            return 0

        lax.fori_loop(1, windows_of(c), some, 0)

    def update(c, rows):
        for j in range(CHUNK):
            to = row(src_ref[c * CHUNK + j])
            ref = sums[j % STREAMS]
            ref[to, :] = ref[to, :] + rows[j : j + 1, :]

    even[...] = expand(0, 0)
    expand_more(0, even)

    def backward(i, _):
        c = 2 * i
        odd[...] = expand(c + 1, 0)
        update(c, even)
        expand_more(c + 1, odd)
        after = jnp.minimum(c + 2, last_chunk)
        even[...] = expand(after, 0)
        update(c + 1, odd)
        expand_more(after, even)
        return 0

    lax.fori_loop(0, pairs, backward, 0)

    def own_part(i, _):
        at = tile(i, step)
        own_ref[at, :] += total(sums, at)
        return 0

    lax.fori_loop(0, local // step, own_part, 0)

    def halo_part(i, _):
        at = pl.ds(pl.multiple_of(local + i * 16 * slots, 8), 16 * slots)
        part = total(sums, at).reshape(16, slots, width).astype(BF16)
        halo_back_ref[pl.ds(i * 16, 16)] = part
        return 0

    lax.fori_loop(0, peers // 16, halo_part, 0)

    clear((hub_slots,), peers * HUB_MOST, 64)

    def hub_part(i, _):
        at = pl.ds(pl.multiple_of(halo_end + i * 8, 8), 8)
        table[tile(i, 8), :] = total(sums, at)
        return 0

    lax.fori_loop(0, hubs // 8, hub_part, 0)

    def hub_out(h, slot):
        hub_slots[row(slot), :] = table[row(h), :]

    each_hub(hub_ref, local, peers // PLANE, hub_out)

    def hub_pack(i, _):
        part = hub_slots[tile(i, 16 * HUB_MOST), :].reshape(16, HUB_MOST, width).astype(BF16)
        hub_back_ref[pl.ds(i * 16, 16)] = part
        return 0

    lax.fori_loop(0, peers // 16, hub_pack, 0)


def final_kernel(hub_ref, send_ref, own_ref, returned_ref, hub_sum, out_ref, rows, parts, sums):
    peers, slots, width = returned_ref.shape
    local = own_ref.shape[0]
    step = 256
    widen(returned_ref, rows, 0)
    for c in range(slots):
        parts[c] = rows[pl.ds(c, peers, stride=slots), :].astype(BF16)

    def some(i, _):
        at = tile(i, step)
        acc = own_ref[at, :]
        for c in range(slots):
            ends = send_ref[c : c + 1, :] - i * step
            hit = lax.broadcasted_iota(jnp.int32, (step, peers), 0) == ends
            pick = jnp.where(hit, 1.0, 0.0).astype(BF16)
            acc = acc + jnp.dot(pick, parts[c], preferred_element_type=F32)
        sums[at, :] = acc
        return 0

    lax.fori_loop(0, local // step, some, 0)
    for j in range(HUB_MOST):
        to = row(hub_ref[j])
        sums[to, :] = sums[to, :] + hub_sum[j : j + 1, :]

    def close(i, _):
        out_ref[tile(i, step), :] = sums[tile(i, step), :].astype(BF16)
        return 0

    lax.fori_loop(0, local // step, close, 0)


PLANE = 32
MESH = pl.DeviceIdType.MESH


class Places:
    def __init__(self):
        self.count = lax.axis_size("vert")
        self.planes = self.count // PLANE
        self.me = lax.axis_index("vert")
        self.z = lax.div(self.me, PLANE)
        self.p = lax.rem(self.me, PLANE)

    def in_plane(self, i):
        p = lax.rem(self.p + i, PLANE)
        return p, self.z * PLANE + p

    def in_line(self, i):
        z = lax.rem(self.z + i, self.planes)
        return z, z * PLANE + self.p

    def barrier(self, ready):
        entry = pltpu.get_barrier_semaphore()

        def greet_plane(i, _):
            pl.semaphore_signal(entry, device_id=(self.in_plane(i)[1],), device_id_type=MESH)
            return 0

        def greet_line(i, _):
            pl.semaphore_signal(entry, device_id=(self.in_line(i)[1],), device_id_type=MESH)
            return 0

        def vouch(i, _):
            pl.semaphore_signal(ready, device_id=(self.in_line(i)[1],), device_id_type=MESH)
            return 0

        lax.fori_loop(1, PLANE, greet_plane, 0)
        lax.fori_loop(1, self.planes, greet_line, 0)
        pl.semaphore_wait(entry, PLANE + self.planes - 2)
        lax.fori_loop(1, self.planes, vouch, 0)
        pl.semaphore_wait(ready, self.planes - 1)

    def copy(self, src, dst, sems, to):
        return pltpu.make_async_remote_copy(
            src_ref=src,
            dst_ref=dst,
            send_sem=sems.at[0],
            recv_sem=sems.at[1],
            device_id=(to,),
            device_id_type=MESH,
        )

    def all_of(self, ref, sems):
        return self.copy(ref, ref, sems, lax.rem(self.me + 1, self.count))

    def send_blocks(self, src, dst, sems, start, stop):
        def some(k, _):
            t = lax.rem(self.me * 75 + k * 159, self.count)

            @pl.when(t != self.me)
            def _():
                self.copy(src.at[t], dst.at[self.me], sems, t).start()

            return 0

        lax.fori_loop(start, stop, some, 0)


def forward_kernel(sent_ref, hub_ref, halo_ref, hubs_ref, a, b, c, keep, ready):
    here = Places()
    here.barrier(ready)
    own_hub = pltpu.make_async_copy(hub_ref, hubs_ref.at[here.p, here.z], keep.at[0])
    own_hub.start()
    own_halo = pltpu.make_async_copy(sent_ref.at[here.me], halo_ref.at[here.me], keep.at[1])
    own_halo.start()

    def along(i, _):
        here.copy(hub_ref, hubs_ref.at[here.p, here.z], a, here.in_line(i)[1]).start()
        return 0

    lax.fori_loop(1, here.planes, along, 0)
    here.send_blocks(sent_ref, halo_ref, b, 0, here.count // 2)
    own_hub.wait()
    here.all_of(hubs_ref.at[here.p, pl.ds(0, here.planes - 1)], a).wait()

    def across(i, _):
        here.copy(hubs_ref.at[here.p], hubs_ref.at[here.p], c, here.in_plane(i)[1]).start()
        return 0

    lax.fori_loop(1, PLANE, across, 0)
    here.send_blocks(sent_ref, halo_ref, b, here.count // 2, here.count)
    own_halo.wait()
    here.all_of(hubs_ref.at[pl.ds(0, PLANE - 1)], c).wait()
    here.all_of(halo_ref.at[pl.ds(0, here.count - 1)], b).wait()


def backward_kernel(
    back_ref, hub_ref, grads_ref, halo_ref, hub_sum_ref, whole_ref,
    part_in, hub_in, grads_in, hub_part, hub_line, grad_part, grad_line,
    a, b, c, d, e, f, keep, ready,
):
    here = Places()
    part_in[...] = grads_ref[...].astype(BF16)
    here.barrier(ready)
    kept = [
        pltpu.make_async_copy(back_ref.at[here.me], halo_ref.at[here.me], keep.at[0]),
        pltpu.make_async_copy(hub_ref.at[here.p], hub_in.at[here.p], keep.at[1]),
        pltpu.make_async_copy(part_in.at[here.p], grads_in.at[here.p], keep.at[2]),
    ]
    for copy in kept:
        copy.start()

    def across(i, _):
        p, to = here.in_plane(i)
        here.copy(part_in.at[p], grads_in.at[here.p], a, to).start()
        here.copy(hub_ref.at[p], hub_in.at[here.p], b, to).start()
        return 0

    lax.fori_loop(1, PLANE, across, 0)
    third = here.count // 3
    here.send_blocks(back_ref, halo_ref, c, 0, third)
    for copy in kept:
        copy.wait()
    here.all_of(grads_in.at[pl.ds(0, PLANE - 1)], a).wait()
    here.all_of(hub_in.at[pl.ds(0, PLANE - 1)], b).wait()
    grad_part[...] = lax.fori_loop(
        0, PLANE, lambda i, acc: acc + grads_in[i].astype(F32), jnp.zeros(grad_part.shape, F32)
    )
    hub_part[...] = lax.fori_loop(
        0, PLANE, lambda i, acc: acc + hub_in[i].astype(F32), jnp.zeros(hub_part.shape, F32)
    )
    here.send_blocks(back_ref, halo_ref, c, third, third + 8)
    kept = [
        pltpu.make_async_copy(grad_part, grad_line.at[here.z], keep.at[0]),
        pltpu.make_async_copy(hub_part.at[here.z], hub_line.at[here.z], keep.at[1]),
    ]
    for copy in kept:
        copy.start()

    def along(i, _):
        z, to = here.in_line(i)
        here.copy(grad_part, grad_line.at[here.z], d, to).start()
        here.copy(hub_part.at[z], hub_line.at[here.z], e, to).start()
        return 0

    lax.fori_loop(1, here.planes, along, 0)
    here.send_blocks(back_ref, halo_ref, c, third + 8, 2 * third)
    for copy in kept:
        copy.wait()
    here.all_of(grad_line.at[pl.ds(0, here.planes - 1)], d).wait()
    here.all_of(hub_line.at[pl.ds(0, here.planes - 1)], e).wait()
    whole = grad_line[0]
    hub_sum = hub_line[0]
    for i in range(1, here.planes):
        whole = whole + grad_line[i]
        hub_sum = hub_sum + hub_line[i]
    grad_part[...] = whole
    hub_sum_ref[...] = hub_sum
    here.send_blocks(back_ref, halo_ref, c, 2 * third, 2 * third + 8)
    kept = pltpu.make_async_copy(grad_part, whole_ref.at[here.p], keep.at[0])
    kept.start()

    def spread(i, _):
        here.copy(grad_part, whole_ref.at[here.p], f, here.in_plane(i)[1]).start()
        return 0

    lax.fori_loop(1, PLANE, spread, 0)
    here.send_blocks(back_ref, halo_ref, c, 2 * third + 8, here.count)
    kept.wait()
    here.all_of(whole_ref.at[pl.ds(0, PLANE - 1)], f).wait()
    here.all_of(halo_ref.at[pl.ds(0, here.count - 1)], c).wait()


def body(
    feats, w_self, w_neigh, bias, cotangent, send_rows, hub_ids, edge_src, edge_dst, edge_count
):
    local, width = feats.shape
    wide = w_self.shape[1]
    peers = lax.axis_size("vert")
    slots = send_rows.shape[2]
    hub_total = hub_ids.shape[0]
    table_rows = local + peers * slots + hub_total
    params = pltpu.CompilerParams(vmem_limit_bytes=LIMIT)

    send = send_rows[0].T
    planes = peers // PLANE

    sent, own_rows, own_back = pl.pallas_call(
        gather_kernel,
        out_shape=(
            jax.ShapeDtypeStruct((peers, slots, width), BF16),
            jax.ShapeDtypeStruct((HUB_MOST, width), BF16),
            jax.ShapeDtypeStruct((HUB_MOST,), jnp.int32),
        ),
        in_specs=[SMEM, SMEM, VMEM],
        out_specs=(VMEM, VMEM, SMEM),
        scratch_shapes=[
            pltpu.VMEM((local, width), F32),
            pltpu.VMEM((peers * slots, width), F32),
        ],
        compiler_params=params,
        name="gather_sent",
    )(hub_ids, send, feats)
    pair = pltpu.SemaphoreType.DMA((2,))
    halo, hubs = pl.pallas_call(
        forward_kernel,
        out_shape=(
            jax.ShapeDtypeStruct((peers, slots, width), BF16),
            jax.ShapeDtypeStruct((PLANE, planes, HUB_MOST, width), BF16),
        ),
        in_specs=[VMEM, VMEM],
        out_specs=(VMEM, VMEM),
        scratch_shapes=[pair] * 4 + [pltpu.SemaphoreType.REGULAR],
        compiler_params=pltpu.CompilerParams(
            vmem_limit_bytes=LIMIT, collective_id=0, has_side_effects=True
        ),
        name="forward_exchange",
    )(sent, own_rows)
    hubs = hubs.reshape(peers, HUB_MOST, width)

    rows_up = up(table_rows, 64)
    output, own, halo_back, hub_back, grads = pl.pallas_call(
        layer_kernel,
        out_shape=(
            jax.ShapeDtypeStruct((local, wide), BF16),
            jax.ShapeDtypeStruct((local, width), F32),
            jax.ShapeDtypeStruct((peers, slots, width), BF16),
            jax.ShapeDtypeStruct((peers, HUB_MOST, width), BF16),
            jax.ShapeDtypeStruct((2 * width, wide + width), F32),
        ),
        in_specs=[SMEM] * 4 + [VMEM] * 8,
        out_specs=(VMEM,) * 5,
        scratch_shapes=[
            pltpu.VMEM((rows_up, width), F32),
            pltpu.VMEM((peers * HUB_MOST, width), F32),
        ]
        + [pltpu.VMEM((local + WINDOW, width), F32)] * 3
        + [pltpu.VMEM((CHUNK, width), F32)] * 2
        + [pltpu.VMEM((rows_up, width), F32)] * STREAMS,
        compiler_params=params,
        name="layer",
    )(
        edge_count, edge_src[0], edge_dst[0], hub_ids, edge_dst.reshape(-1, 128), feats,
        halo, hubs, cotangent, w_self, w_neigh, bias[None, :],
    )

    piece = (2 * width // PLANE, wide + width)
    returned, hub_sum, whole = pl.pallas_call(
        backward_kernel,
        out_shape=(
            jax.ShapeDtypeStruct((peers, slots, width), BF16),
            jax.ShapeDtypeStruct((HUB_MOST, width), F32),
            jax.ShapeDtypeStruct((PLANE,) + piece, F32),
        ),
        in_specs=[VMEM] * 3,
        out_specs=(VMEM,) * 3,
        scratch_shapes=[
            pltpu.VMEM((PLANE,) + piece, BF16),
            pltpu.VMEM((PLANE, planes, HUB_MOST, width), BF16),
            pltpu.VMEM((PLANE,) + piece, BF16),
            pltpu.VMEM((planes, HUB_MOST, width), F32),
            pltpu.VMEM((planes, HUB_MOST, width), F32),
            pltpu.VMEM(piece, F32),
            pltpu.VMEM((planes,) + piece, F32),
        ]
        + [pair] * 6
        + [pltpu.SemaphoreType.DMA((3,)), pltpu.SemaphoreType.REGULAR],
        compiler_params=pltpu.CompilerParams(
            vmem_limit_bytes=LIMIT, collective_id=1, has_side_effects=True
        ),
        name="backward_exchange",
    )(
        halo_back,
        hub_back.reshape(PLANE, planes, HUB_MOST, width),
        grads.reshape((PLANE,) + piece),
    )
    whole = whole.reshape(2 * width, wide + width)
    grad_feats = pl.pallas_call(
        final_kernel,
        out_shape=jax.ShapeDtypeStruct((local, width), BF16),
        in_specs=[SMEM] + [VMEM] * 4,
        out_specs=VMEM,
        scratch_shapes=[
            pltpu.VMEM((peers * slots, width), F32),
            pltpu.VMEM((slots, peers, width), BF16),
            pltpu.VMEM((up(local + 1, 8), width), F32),
        ],
        compiler_params=params,
        name="final",
    )(own_back, send, own, returned, hub_sum)
    grad_bias = jnp.concatenate(
        [jnp.sum(whole[8 * j : 8 * j + 8, wide:], axis=0) for j in range(wide // width)]
    )
    return (output, grad_feats, whole[:width, :wide], whole[width:, :wide], grad_bias)


def solution(mesh):
    in_specs = (
        P("vert", None),
        P(),
        P(),
        P(),
        P("vert", None),
        P("vert", None, None),
        P(),
        P("vert", None),
        P("vert", None),
        P("vert"),
    )
    out_specs = (P("vert", None), P("vert", None), P(), P(), P())
    return jax.shard_map(body, mesh=mesh, in_specs=in_specs, out_specs=out_specs, check_vma=False)
```

```python
import functools

import jax
import jax.numpy as jnp
from jax import lax
from jax.experimental import pallas as pl
from jax.experimental.pallas import tpu as pltpu
from jax.sharding import PartitionSpec as P

HUB_MOST = 8
STREAMS = 8
GROUP = 32
CHUNK = 256
WINDOW = 64
FIRST = 168
SECOND = 232
LIMIT = 60 * 1024 * 1024
F32 = jnp.float32
BF16 = jnp.bfloat16
SMEM = pl.BlockSpec(memory_space=pltpu.SMEM)
VMEM = pl.BlockSpec(memory_space=pltpu.VMEM)


def up(n, k):
    return -(-n // k) * k


def row(i):
    return pl.ds(i, 1)


def tile(i, step):
    return pl.ds(pl.multiple_of(i * step, step), step)


def clear(refs, rows, step):
    def some(i, _):
        for ref in refs:
            ref[tile(i, step), :] = jnp.zeros((step, ref.shape[1]), F32)
        return 0

    lax.fori_loop(0, rows // step, some, 0)


def total(sums, at):
    parts = [ref[at, :] for ref in sums]
    while len(parts) > 1:
        parts = [a + b for a, b in zip(parts[::2], parts[1::2])]
    return parts[0]


def widen(ref, table, start):
    blocks, slots = 16, ref.shape[1]

    def some(i, _):
        part = ref[pl.ds(i * blocks, blocks)]
        at = pl.multiple_of(start + i * blocks * slots, 8)
        table[pl.ds(at, blocks * slots), :] = part.astype(F32).reshape(blocks * slots, -1)
        return 0

    lax.fori_loop(0, ref.shape[0] // blocks, some, 0)


def each_hub(hub_ref, local, planes, visit):
    shift = local.bit_length() - 1

    def some(i, carry):
        last, offset = carry
        for j in range(8):
            h = i * 8 + j
            owner = hub_ref[h] >> shift
            offset = jnp.where(owner == last, offset + 1, 0)
            block = lax.rem(owner, PLANE) * planes + lax.div(owner, PLANE)
            visit(h, block * HUB_MOST + offset)
            last = owner
        return last, offset

    lax.fori_loop(0, hub_ref.shape[0] // 8, some, (jnp.int32(-1), jnp.int32(0)))


def gather_kernel(hub_ref, send_ref, feats_ref, out_ref, hub_out_ref, back_ref, table, rows):
    peers, slots, width = out_ref.shape
    local = feats_ref.shape[0]
    hubs = hub_ref.shape[0]
    table[...] = feats_ref[...].astype(F32)

    def some(i, _):
        for j in range(GROUP):
            p, c = i * (GROUP // slots) + j // slots, j % slots
            rows[row(i * GROUP + j), :] = table[row(send_ref[c, p]), :]
        return 0

    lax.fori_loop(0, peers * slots // GROUP, some, 0)
    start = lax.axis_index("vert") * local

    def look(i, carry):
        first, after = carry
        for j in range(8):
            at = hub_ref[i * 8 + j] - start
            first = first + (at < 0).astype(jnp.int32)
            after = after + (at < local).astype(jnp.int32)
        return first, after

    first, after = lax.fori_loop(0, hubs // 8, look, (jnp.int32(0), jnp.int32(0)))
    own = []
    for j in range(HUB_MOST):
        here = jnp.minimum(first + j, jnp.maximum(after - 1, 0))
        at = jnp.clip(hub_ref[here] - start, 0, local - 1)
        own.append(table[row(at), :])
        back_ref[j] = jnp.where(first + j < after, at, local)
    back_ref[HUB_MOST] = first
    hub_out_ref[...] = jnp.concatenate(own, axis=0).astype(BF16)

    def pack(i, _):
        part = rows[tile(i, 16 * slots), :].reshape(16, slots, width).astype(BF16)
        out_ref[pl.ds(i * 16, 16)] = part
        return 0

    lax.fori_loop(0, peers // 16, pack, 0)


def one_hot(lanes_ref, c, base, count):
    halves = []
    for h in range(CHUNK // 128):
        r = c * (CHUNK // 128) + h
        ends = lanes_ref[row(r), :] - base
        e = r * 128 + lax.broadcasted_iota(jnp.int32, (1, 128), 1)
        ends = jnp.where(e < count, ends, -1)
        hit = lax.broadcasted_iota(jnp.int32, (WINDOW, 128), 0) == ends
        halves.append(jnp.where(hit, 1.0, 0.0).astype(BF16))
    return jnp.concatenate(halves, axis=1)


def layer_kernel(
    count_ref, src_ref, dst_ref, hub_ref,
    lanes_ref, feats_ref, halo_ref, hubs_ref, cot_ref, w_self_ref, w_neigh_ref, bias_ref,
    out_ref, own_ref, halo_back_ref, grads_ref,
    table, hub_slots, spread, summed, degrees, even, odd, *sums,
):
    local, width = feats_ref.shape
    peers, slots, _ = halo_ref.shape
    hubs = hub_ref.shape[0]
    wide = w_self_ref.shape[1]
    halo_end = local + peers * slots
    last_chunk = src_ref.shape[0] // CHUNK - 1
    count = count_ref[0]
    pairs = lax.div(count + (2 * CHUNK - 1), 2 * CHUNK)
    step = 256
    outer = (((0,), (0,)), ((), ()))
    back = (((1,), (1,)), ((), ()))

    def base_of(c):
        return lax.shift_left(lax.shift_right_logical(dst_ref[c * CHUNK], 3), 3)

    def windows_of(c):
        return lax.div(dst_ref[c * CHUNK + CHUNK - 1] - base_of(c), WINDOW) + 1

    clear((summed, degrees), summed.shape[0], WINDOW)
    table[:local, :] = feats_ref[...].astype(F32)
    widen(halo_ref, table, local)
    widen(hubs_ref, hub_slots, 0)

    def hub_in(h, slot):
        table[row(halo_end + h), :] = hub_slots[row(slot), :]

    each_hub(hub_ref, local, peers // PLANE, hub_in)

    def fetch(c, rows):
        for j in range(CHUNK):
            rows[j : j + 1, :] = table[row(src_ref[c * CHUNK + j]), :]

    def reduce(c, rows, k):
        base = pl.multiple_of(base_of(c) + k * WINDOW, 8)
        at = pl.ds(base, WINDOW)
        right = jnp.concatenate([rows[...].astype(BF16), jnp.ones((CHUNK, width), BF16)], axis=1)
        part = jnp.dot(one_hot(lanes_ref, c, base, count), right, preferred_element_type=F32)
        summed[at, :] += part[:, :width]
        degrees[at, :] += part[:, width:]

    def reduce_more(c, rows):
        def some(k, _):
            reduce(c, rows, k)
            return 0

        lax.fori_loop(1, windows_of(c), some, 0)

    fetch(0, even)

    def forward(i, _):
        c = 2 * i
        reduce(c, even, 0)
        fetch(c + 1, odd)
        reduce_more(c, even)
        reduce(c + 1, odd, 0)
        fetch(jnp.minimum(c + 2, last_chunk), even)
        reduce_more(c + 1, odd)
        return 0

    lax.fori_loop(0, pairs, forward, 0)

    grads_ref[...] = jnp.zeros_like(grads_ref)
    w_self, w_neigh, bias = w_self_ref[...], w_neigh_ref[...], bias_ref[...]

    def dense(i, _):
        at = tile(i, step)
        feats = feats_ref[at, :]
        inverse = 1.0 / jnp.maximum(degrees[at, :], 1.0)
        mean = (summed[at, :] * inverse).astype(BF16)
        linear = jnp.dot(feats, w_self, preferred_element_type=F32)
        linear = linear + jnp.dot(mean, w_neigh, preferred_element_type=F32) + bias
        logistic = jax.nn.sigmoid(linear)
        out_ref[at, :] = (linear * logistic).astype(BF16)
        slope = logistic * (1.0 + linear * (1.0 - logistic))
        grad = (cot_ref[at, :].astype(F32) * slope).astype(BF16)
        grads_ref[:width, :wide] += lax.dot_general(feats, grad, outer, preferred_element_type=F32)
        grads_ref[width : 2 * width, :wide] += lax.dot_general(
            mean, grad, outer, preferred_element_type=F32
        )
        grad_sum = jnp.sum(grad.astype(F32).reshape(step // 8, 8, wide), axis=0)
        for j in range(wide // width):
            grads_ref[8 * j : 8 * j + 8, wide : wide + width] += grad_sum[:, j * width : (j + 1) * width]
        own_ref[at, :] = lax.dot_general(grad, w_self, back, preferred_element_type=F32)
        spread[at, :] = lax.dot_general(grad, w_neigh, back, preferred_element_type=F32) * inverse
        return 0

    lax.fori_loop(0, local // step, dense, 0)

    clear(sums, sums[0].shape[0], 64)
    spread[local:, :] = jnp.zeros((spread.shape[0] - local, width), F32)

    def expand(c, k):
        base = pl.multiple_of(base_of(c) + k * WINDOW, 8)
        values = spread[pl.ds(base, WINDOW), :]
        high = values.astype(BF16)
        low = (values - high.astype(F32)).astype(BF16)
        both = lax.dot_general(
            one_hot(lanes_ref, c, base, count),
            jnp.concatenate([high, low], axis=1),
            outer,
            preferred_element_type=F32,
        )
        return both[:, :width] + both[:, width:]

    def expand_more(c, rows):
        def some(k, _):
            rows[...] += expand(c, k)
            return 0

        lax.fori_loop(1, windows_of(c), some, 0)

    def update(c, rows):
        for j in range(CHUNK):
            to = row(src_ref[c * CHUNK + j])
            ref = sums[j % STREAMS]
            ref[to, :] = ref[to, :] + rows[j : j + 1, :]

    even[...] = expand(0, 0)
    expand_more(0, even)

    def backward(i, _):
        c = 2 * i
        odd[...] = expand(c + 1, 0)
        update(c, even)
        expand_more(c + 1, odd)
        after = jnp.minimum(c + 2, last_chunk)
        even[...] = expand(after, 0)
        update(c + 1, odd)
        expand_more(after, even)
        return 0

    lax.fori_loop(0, pairs, backward, 0)

    def own_part(i, _):
        at = tile(i, step)
        own_ref[at, :] += total(sums, at)
        return 0

    lax.fori_loop(0, local // step, own_part, 0)

    def halo_part(i, _):
        at = pl.ds(pl.multiple_of(local + i * 16 * slots, 8), 16 * slots)
        part = total(sums, at).reshape(16, slots, width).astype(BF16)
        halo_back_ref[pl.ds(i * 16, 16)] = part
        return 0

    lax.fori_loop(0, peers // 16, halo_part, 0)

    def hub_part(i, _):
        for j in range(2):
            at = pl.ds(pl.multiple_of(halo_end + i * 16 + j * 8, 8), 8)
            lanes = wide + (1 + j) * width
            grads_ref[tile(i, 8), lanes : lanes + width] = total(sums, at)
        return 0

    lax.fori_loop(0, hubs // 16, hub_part, 0)


def final_kernel(hub_ref, send_ref, own_ref, returned_ref, whole_ref, out_ref, rows, parts, sums):
    peers, slots, width = returned_ref.shape
    local = own_ref.shape[0]
    step = 256
    widen(returned_ref, rows, 0)
    for c in range(slots):
        parts[c] = rows[pl.ds(c, peers, stride=slots), :].astype(BF16)

    def some(i, _):
        at = tile(i, step)
        acc = own_ref[at, :]
        for c in range(slots):
            ends = send_ref[c : c + 1, :] - i * step
            hit = lax.broadcasted_iota(jnp.int32, (step, peers), 0) == ends
            pick = jnp.where(hit, 1.0, 0.0).astype(BF16)
            acc = acc + jnp.dot(pick, parts[c], preferred_element_type=F32)
        sums[at, :] = acc
        return 0

    lax.fori_loop(0, local // step, some, 0)
    lanes = whole_ref.shape[1] - 2 * width
    for j in range(HUB_MOST):
        to = row(hub_ref[j])
        h = hub_ref[HUB_MOST] + j
        both = whole_ref[row(lax.div(h, 16) * 8 + lax.rem(h, 8)), lanes:]
        late = lax.rem(h, 16) >= 8
        sums[to, :] = sums[to, :] + jnp.where(late, both[:, width:], both[:, :width])

    def close(i, _):
        out_ref[tile(i, step), :] = sums[tile(i, step), :].astype(BF16)
        return 0

    lax.fori_loop(0, local // step, close, 0)


PLANE = 32
MESH = pl.DeviceIdType.MESH


class Places:
    def __init__(self):
        self.count = lax.axis_size("vert")
        self.planes = self.count // PLANE
        self.me = lax.axis_index("vert")
        self.z = lax.div(self.me, PLANE)
        self.p = lax.rem(self.me, PLANE)

    def in_plane(self, i):
        p = lax.rem(self.p + i, PLANE)
        return p, self.z * PLANE + p

    def in_line(self, i):
        z = lax.rem(self.z + i, self.planes)
        return z, z * PLANE + self.p

    def barrier(self, ready):
        entry = pltpu.get_barrier_semaphore()

        def greet_plane(i, _):
            pl.semaphore_signal(entry, device_id=(self.in_plane(i)[1],), device_id_type=MESH)
            return 0

        def greet_line(i, _):
            pl.semaphore_signal(entry, device_id=(self.in_line(i)[1],), device_id_type=MESH)
            return 0

        def vouch(i, _):
            pl.semaphore_signal(ready, device_id=(self.in_line(i)[1],), device_id_type=MESH)
            return 0

        lax.fori_loop(1, PLANE, greet_plane, 0)
        lax.fori_loop(1, self.planes, greet_line, 0)
        pl.semaphore_wait(entry, PLANE + self.planes - 2)
        lax.fori_loop(1, self.planes, vouch, 0)
        pl.semaphore_wait(ready, self.planes - 1)

    def copy(self, src, dst, sems, to):
        return pltpu.make_async_remote_copy(
            src_ref=src,
            dst_ref=dst,
            send_sem=sems.at[0],
            recv_sem=sems.at[1],
            device_id=(to,),
            device_id_type=MESH,
        )

    def all_of(self, ref, sems):
        return self.copy(ref, ref, sems, lax.rem(self.me + 1, self.count))

    def send_blocks(self, src, dst, sems, start, stop):
        def some(k, _):
            t = lax.rem(self.me * 75 + k * 159, self.count)

            @pl.when(t != self.me)
            def _():
                self.copy(src.at[t], dst.at[self.me], sems, t).start()

            return 0

        lax.fori_loop(start, stop, some, 0)


def forward_kernel(sent_ref, hub_ref, halo_ref, hubs_ref, a, b, c, keep, ready):
    here = Places()
    here.barrier(ready)
    own_hub = pltpu.make_async_copy(hub_ref, hubs_ref.at[here.p, here.z], keep.at[0])
    own_hub.start()
    own_halo = pltpu.make_async_copy(sent_ref.at[here.me], halo_ref.at[here.me], keep.at[1])
    own_halo.start()

    def along(i, _):
        here.copy(hub_ref, hubs_ref.at[here.p, here.z], a, here.in_line(i)[1]).start()
        return 0

    lax.fori_loop(1, here.planes, along, 0)
    here.send_blocks(sent_ref, halo_ref, b, 0, here.count // 2)
    own_hub.wait()
    here.all_of(hubs_ref.at[here.p, pl.ds(0, here.planes - 1)], a).wait()

    def across(i, _):
        here.copy(hubs_ref.at[here.p], hubs_ref.at[here.p], c, here.in_plane(i)[1]).start()
        return 0

    lax.fori_loop(1, PLANE, across, 0)
    here.send_blocks(sent_ref, halo_ref, b, here.count // 2, here.count)
    own_halo.wait()
    here.all_of(hubs_ref.at[pl.ds(0, PLANE - 1)], c).wait()
    here.all_of(halo_ref.at[pl.ds(0, here.count - 1)], b).wait()


def backward_kernel(
    back_ref, grads_ref, halo_ref, whole_ref, part_in, parts, part, line, a, b, c, d, keep, ready
):
    here = Places()
    part_in[...] = grads_ref[...].astype(BF16)
    here.barrier(ready)
    kept = [
        pltpu.make_async_copy(back_ref.at[here.me], halo_ref.at[here.me], keep.at[0]),
        pltpu.make_async_copy(part_in.at[here.p], parts.at[here.p], keep.at[1]),
    ]
    for copy in kept:
        copy.start()

    def across(i, _):
        p, to = here.in_plane(i)
        here.copy(part_in.at[p], parts.at[here.p], a, to).start()
        return 0

    lax.fori_loop(1, PLANE, across, 0)
    early, later = here.count * FIRST // 256, here.count * SECOND // 256
    here.send_blocks(back_ref, halo_ref, b, 0, early)
    for copy in kept:
        copy.wait()
    here.all_of(parts.at[pl.ds(0, PLANE - 1)], a).wait()
    part[...] = lax.fori_loop(
        0, PLANE, lambda i, acc: acc + parts[i].astype(F32), jnp.zeros(part.shape, F32)
    )
    here.send_blocks(back_ref, halo_ref, b, early, early + 8)
    kept = pltpu.make_async_copy(part, line.at[here.z], keep.at[0])
    kept.start()

    def along(i, _):
        here.copy(part, line.at[here.z], c, here.in_line(i)[1]).start()
        return 0

    lax.fori_loop(1, here.planes, along, 0)
    here.send_blocks(back_ref, halo_ref, b, early + 8, later)
    kept.wait()
    here.all_of(line.at[pl.ds(0, here.planes - 1)], c).wait()
    whole = line[0]
    for i in range(1, here.planes):
        whole = whole + line[i]
    part[...] = whole
    here.send_blocks(back_ref, halo_ref, b, later, later + 8)
    kept = pltpu.make_async_copy(part, whole_ref.at[here.p], keep.at[0])
    kept.start()

    def spread(i, _):
        here.copy(part, whole_ref.at[here.p], d, here.in_plane(i)[1]).start()
        return 0

    lax.fori_loop(1, PLANE, spread, 0)
    here.send_blocks(back_ref, halo_ref, b, later + 8, here.count)
    kept.wait()
    here.all_of(whole_ref.at[pl.ds(0, PLANE - 1)], d).wait()
    here.all_of(halo_ref.at[pl.ds(0, here.count - 1)], b).wait()


def body(
    feats, w_self, w_neigh, bias, cotangent, send_rows, hub_ids, edge_src, edge_dst, edge_count
):
    local, width = feats.shape
    wide = w_self.shape[1]
    peers = lax.axis_size("vert")
    slots = send_rows.shape[2]
    hub_total = hub_ids.shape[0]
    table_rows = local + peers * slots + hub_total
    params = pltpu.CompilerParams(vmem_limit_bytes=LIMIT)

    send = send_rows[0].T
    planes = peers // PLANE

    sent, own_rows, own_back = pl.pallas_call(
        gather_kernel,
        out_shape=(
            jax.ShapeDtypeStruct((peers, slots, width), BF16),
            jax.ShapeDtypeStruct((HUB_MOST, width), BF16),
            jax.ShapeDtypeStruct((HUB_MOST + 1,), jnp.int32),
        ),
        in_specs=[SMEM, SMEM, VMEM],
        out_specs=(VMEM, VMEM, SMEM),
        scratch_shapes=[
            pltpu.VMEM((local, width), F32),
            pltpu.VMEM((peers * slots, width), F32),
        ],
        compiler_params=params,
        name="gather_sent",
    )(hub_ids, send, feats)
    pair = pltpu.SemaphoreType.DMA((2,))
    halo, hubs = pl.pallas_call(
        forward_kernel,
        out_shape=(
            jax.ShapeDtypeStruct((peers, slots, width), BF16),
            jax.ShapeDtypeStruct((PLANE, planes, HUB_MOST, width), BF16),
        ),
        in_specs=[VMEM, VMEM],
        out_specs=(VMEM, VMEM),
        scratch_shapes=[pair] * 4 + [pltpu.SemaphoreType.REGULAR],
        compiler_params=pltpu.CompilerParams(
            vmem_limit_bytes=LIMIT, collective_id=0, has_side_effects=True
        ),
        name="forward_exchange",
    )(sent, own_rows)
    hubs = hubs.reshape(peers, HUB_MOST, width)

    rows_up = up(table_rows, 64)
    output, own, halo_back, grads = pl.pallas_call(
        layer_kernel,
        out_shape=(
            jax.ShapeDtypeStruct((local, wide), BF16),
            jax.ShapeDtypeStruct((local, width), F32),
            jax.ShapeDtypeStruct((peers, slots, width), BF16),
            jax.ShapeDtypeStruct((2 * width, wide + 3 * width), F32),
        ),
        in_specs=[SMEM] * 4 + [VMEM] * 8,
        out_specs=(VMEM,) * 4,
        scratch_shapes=[
            pltpu.VMEM((rows_up, width), F32),
            pltpu.VMEM((peers * HUB_MOST, width), F32),
        ]
        + [pltpu.VMEM((local + WINDOW, width), F32)] * 3
        + [pltpu.VMEM((CHUNK, width), F32)] * 2
        + [pltpu.VMEM((rows_up, width), F32)] * STREAMS,
        compiler_params=params,
        name="layer",
    )(
        edge_count, edge_src[0], edge_dst[0], hub_ids, edge_dst.reshape(-1, 128), feats,
        halo, hubs, cotangent, w_self, w_neigh, bias[None, :],
    )

    piece = (2 * width // PLANE, wide + 3 * width)
    returned, whole = pl.pallas_call(
        backward_kernel,
        out_shape=(
            jax.ShapeDtypeStruct((peers, slots, width), BF16),
            jax.ShapeDtypeStruct((PLANE,) + piece, F32),
        ),
        in_specs=[VMEM] * 2,
        out_specs=(VMEM,) * 2,
        scratch_shapes=[
            pltpu.VMEM((PLANE,) + piece, BF16),
            pltpu.VMEM((PLANE,) + piece, BF16),
            pltpu.VMEM(piece, F32),
            pltpu.VMEM((planes,) + piece, F32),
        ]
        + [pair] * 4
        + [pltpu.SemaphoreType.DMA((2,)), pltpu.SemaphoreType.REGULAR],
        compiler_params=pltpu.CompilerParams(
            vmem_limit_bytes=LIMIT, collective_id=1, has_side_effects=True
        ),
        name="backward_exchange",
    )(halo_back, grads.reshape((PLANE,) + piece))
    whole = whole.reshape(2 * width, wide + 3 * width)
    grad_feats = pl.pallas_call(
        final_kernel,
        out_shape=jax.ShapeDtypeStruct((local, width), BF16),
        in_specs=[SMEM] + [VMEM] * 4,
        out_specs=VMEM,
        scratch_shapes=[
            pltpu.VMEM((peers * slots, width), F32),
            pltpu.VMEM((slots, peers, width), BF16),
            pltpu.VMEM((up(local + 1, 8), width), F32),
        ],
        compiler_params=params,
        name="final",
    )(own_back, send, own, returned, whole)
    grad_bias = jnp.concatenate(
        [jnp.sum(whole[8 * j : 8 * j + 8, wide : wide + width], axis=0) for j in range(wide // width)]
    )
    return (output, grad_feats, whole[:width, :wide], whole[width:, :wide], grad_bias)


def solution(mesh):
    in_specs = (
        P("vert", None),
        P(),
        P(),
        P(),
        P("vert", None),
        P("vert", None, None),
        P(),
        P("vert", None),
        P("vert", None),
        P("vert"),
    )
    out_specs = (P("vert", None), P("vert", None), P(), P(), P())
    return jax.shard_map(body, mesh=mesh, in_specs=in_specs, out_specs=out_specs, check_vma=False)
```

```python
import functools

import jax
import jax.numpy as jnp
from jax import lax
from jax.experimental import pallas as pl
from jax.experimental.pallas import tpu as pltpu
from jax.sharding import PartitionSpec as P

HUB_MOST = 8
STREAMS = 8
GROUP = 32
CHUNK = 256
WINDOW = 64
FIRST = 168
SECOND = 232
LIMIT = 60 * 1024 * 1024
F32 = jnp.float32
BF16 = jnp.bfloat16
SMEM = pl.BlockSpec(memory_space=pltpu.SMEM)
VMEM = pl.BlockSpec(memory_space=pltpu.VMEM)


def up(n, k):
    return -(-n // k) * k


def row(i):
    return pl.ds(i, 1)


def tile(i, step):
    return pl.ds(pl.multiple_of(i * step, step), step)


def clear(refs, rows, step):
    def some(i, _):
        for ref in refs:
            ref[tile(i, step), :] = jnp.zeros((step, ref.shape[1]), F32)
        return 0

    lax.fori_loop(0, rows // step, some, 0)


def total(sums, at):
    parts = [ref[at, :] for ref in sums]
    while len(parts) > 1:
        parts = [a + b for a, b in zip(parts[::2], parts[1::2])]
    return parts[0]


def widen(ref, table, start):
    blocks, slots = 16, ref.shape[1]

    def some(i, _):
        part = ref[pl.ds(i * blocks, blocks)]
        at = pl.multiple_of(start + i * blocks * slots, 8)
        table[pl.ds(at, blocks * slots), :] = part.astype(F32).reshape(blocks * slots, -1)
        return 0

    lax.fori_loop(0, ref.shape[0] // blocks, some, 0)


def each_hub(hub_ref, local, planes, visit):
    shift = local.bit_length() - 1

    def some(i, carry):
        last, offset = carry
        for j in range(8):
            h = i * 8 + j
            owner = hub_ref[h] >> shift
            offset = jnp.where(owner == last, offset + 1, 0)
            block = lax.rem(owner, PLANE) * planes + lax.div(owner, PLANE)
            visit(h, block * HUB_MOST + offset)
            last = owner
        return last, offset

    lax.fori_loop(0, hub_ref.shape[0] // 8, some, (jnp.int32(-1), jnp.int32(0)))


def gather_kernel(hub_ref, send_ref, feats_ref, out_ref, hub_out_ref, back_ref, table, rows):
    peers, slots, width = out_ref.shape
    local = feats_ref.shape[0]
    hubs = hub_ref.shape[0]
    table[...] = feats_ref[...].astype(F32)

    def some(i, _):
        for j in range(GROUP):
            p, c = i * (GROUP // slots) + j // slots, j % slots
            rows[row(i * GROUP + j), :] = table[row(send_ref[c, p]), :]
        return 0

    lax.fori_loop(0, peers * slots // GROUP, some, 0)
    start = lax.axis_index("vert") * local

    def look(i, carry):
        first, after = carry
        for j in range(8):
            at = hub_ref[i * 8 + j] - start
            first = first + (at < 0).astype(jnp.int32)
            after = after + (at < local).astype(jnp.int32)
        return first, after

    first, after = lax.fori_loop(0, hubs // 8, look, (jnp.int32(0), jnp.int32(0)))
    own = []
    for j in range(HUB_MOST):
        here = jnp.minimum(first + j, jnp.maximum(after - 1, 0))
        at = jnp.clip(hub_ref[here] - start, 0, local - 1)
        own.append(table[row(at), :])
        back_ref[j] = jnp.where(first + j < after, at, local)
    back_ref[HUB_MOST] = first
    hub_out_ref[...] = jnp.concatenate(own, axis=0).astype(BF16)

    def pack(i, _):
        part = rows[tile(i, 16 * slots), :].reshape(16, slots, width).astype(BF16)
        out_ref[pl.ds(i * 16, 16)] = part
        return 0

    lax.fori_loop(0, peers // 16, pack, 0)


def one_hot(lanes_ref, c, base, count):
    halves = []
    for h in range(CHUNK // 128):
        r = c * (CHUNK // 128) + h
        ends = lanes_ref[row(r), :] - base
        e = r * 128 + lax.broadcasted_iota(jnp.int32, (1, 128), 1)
        ends = jnp.where(e < count, ends, -1)
        hit = lax.broadcasted_iota(jnp.int32, (WINDOW, 128), 0) == ends
        halves.append(jnp.where(hit, 1.0, 0.0).astype(BF16))
    return jnp.concatenate(halves, axis=1)


def layer_kernel(
    count_ref, src_ref, dst_ref, hub_ref,
    lanes_ref, feats_ref, halo_ref, hubs_ref, cot_ref, w_self_ref, w_neigh_ref, bias_ref,
    out_ref, own_ref, halo_back_ref, grads_ref,
    table, hub_slots, spread, summed, degrees, even, odd, *sums,
):
    local, width = feats_ref.shape
    peers, slots, _ = halo_ref.shape
    hubs = hub_ref.shape[0]
    wide = w_self_ref.shape[1]
    halo_end = local + peers * slots
    last_chunk = src_ref.shape[0] // CHUNK - 1
    count = count_ref[0]
    pairs = lax.div(count + (2 * CHUNK - 1), 2 * CHUNK)
    step = 256
    outer = (((0,), (0,)), ((), ()))
    back = (((1,), (1,)), ((), ()))

    def base_of(c):
        return lax.shift_left(lax.shift_right_logical(dst_ref[c * CHUNK], 3), 3)

    def windows_of(c):
        return lax.div(dst_ref[c * CHUNK + CHUNK - 1] - base_of(c), WINDOW) + 1

    clear((summed, degrees), summed.shape[0], WINDOW)
    table[:local, :] = feats_ref[...].astype(F32)
    widen(halo_ref, table, local)
    widen(hubs_ref, hub_slots, 0)

    def hub_in(h, slot):
        table[row(halo_end + h), :] = hub_slots[row(slot), :]

    each_hub(hub_ref, local, peers // PLANE, hub_in)

    def fetch(c, rows):
        for j in range(CHUNK):
            rows[j : j + 1, :] = table[row(src_ref[c * CHUNK + j]), :]

    def reduce(c, rows, k):
        base = pl.multiple_of(base_of(c) + k * WINDOW, 8)
        at = pl.ds(base, WINDOW)
        right = jnp.concatenate([rows[...].astype(BF16), jnp.ones((CHUNK, width), BF16)], axis=1)
        part = jnp.dot(one_hot(lanes_ref, c, base, count), right, preferred_element_type=F32)
        summed[at, :] += part[:, :width]
        degrees[at, :] += part[:, width:]

    def reduce_more(c, rows):
        def some(k, _):
            reduce(c, rows, k)
            return 0

        lax.fori_loop(1, windows_of(c), some, 0)

    fetch(0, even)

    def forward(i, _):
        c = 2 * i
        reduce(c, even, 0)
        fetch(c + 1, odd)
        reduce_more(c, even)
        reduce(c + 1, odd, 0)
        fetch(jnp.minimum(c + 2, last_chunk), even)
        reduce_more(c + 1, odd)
        return 0

    lax.fori_loop(0, pairs, forward, 0)

    grads_ref[...] = jnp.zeros_like(grads_ref)
    w_self, w_neigh, bias = w_self_ref[...], w_neigh_ref[...], bias_ref[...]

    def dense(i, _):
        at = tile(i, step)
        feats = feats_ref[at, :]
        inverse = 1.0 / jnp.maximum(degrees[at, :], 1.0)
        mean = (summed[at, :] * inverse).astype(BF16)
        linear = jnp.dot(feats, w_self, preferred_element_type=F32)
        linear = linear + jnp.dot(mean, w_neigh, preferred_element_type=F32) + bias
        logistic = jax.nn.sigmoid(linear)
        out_ref[at, :] = (linear * logistic).astype(BF16)
        slope = logistic * (1.0 + linear * (1.0 - logistic))
        grad = (cot_ref[at, :].astype(F32) * slope).astype(BF16)
        grads_ref[:width, :wide] += lax.dot_general(feats, grad, outer, preferred_element_type=F32)
        grads_ref[width : 2 * width, :wide] += lax.dot_general(
            mean, grad, outer, preferred_element_type=F32
        )
        grad_sum = jnp.sum(grad.astype(F32).reshape(step // 8, 8, wide), axis=0)
        grads_ref[2 * width - 8 :, wide:] += grad_sum
        own_ref[at, :] = lax.dot_general(grad, w_self, back, preferred_element_type=F32)
        spread[at, :] = lax.dot_general(grad, w_neigh, back, preferred_element_type=F32) * inverse
        return 0

    lax.fori_loop(0, local // step, dense, 0)

    clear(sums, sums[0].shape[0], 64)
    spread[local:, :] = jnp.zeros((spread.shape[0] - local, width), F32)

    def expand(c, k):
        base = pl.multiple_of(base_of(c) + k * WINDOW, 8)
        values = spread[pl.ds(base, WINDOW), :]
        high = values.astype(BF16)
        low = (values - high.astype(F32)).astype(BF16)
        both = lax.dot_general(
            one_hot(lanes_ref, c, base, count),
            jnp.concatenate([high, low], axis=1),
            outer,
            preferred_element_type=F32,
        )
        return both[:, :width] + both[:, width:]

    def expand_more(c, rows):
        def some(k, _):
            rows[...] += expand(c, k)
            return 0

        lax.fori_loop(1, windows_of(c), some, 0)

    def update(c, rows):
        for j in range(CHUNK):
            to = row(src_ref[c * CHUNK + j])
            ref = sums[j % STREAMS]
            ref[to, :] = ref[to, :] + rows[j : j + 1, :]

    even[...] = expand(0, 0)
    expand_more(0, even)

    def backward(i, _):
        c = 2 * i
        odd[...] = expand(c + 1, 0)
        update(c, even)
        expand_more(c + 1, odd)
        after = jnp.minimum(c + 2, last_chunk)
        even[...] = expand(after, 0)
        update(c + 1, odd)
        expand_more(after, even)
        return 0

    lax.fori_loop(0, pairs, backward, 0)

    def own_part(i, _):
        at = tile(i, step)
        own_ref[at, :] += total(sums, at)
        return 0

    lax.fori_loop(0, local // step, own_part, 0)

    def halo_part(i, _):
        at = pl.ds(pl.multiple_of(local + i * 16 * slots, 8), 16 * slots)
        part = total(sums, at).reshape(16, slots, width).astype(BF16)
        halo_back_ref[pl.ds(i * 16, 16)] = part
        return 0

    lax.fori_loop(0, peers // 16, halo_part, 0)

    def hub_part(i, _):
        for j in range(2):
            at = pl.ds(pl.multiple_of(halo_end + i * 16 + j * 8, 8), 8)
            lanes = wide + j * width
            grads_ref[tile(i, 8), lanes : lanes + width] = total(sums, at)
        return 0

    lax.fori_loop(0, hubs // 16, hub_part, 0)


def final_kernel(
    hub_ref, send_ref, own_ref, returned_ref, whole_ref,
    out_ref, w_self_ref, w_neigh_ref, bias_ref, rows, parts, sums,
):
    peers, slots, width = returned_ref.shape
    local = own_ref.shape[0]
    step = 256
    widen(returned_ref, rows, 0)
    for c in range(slots):
        parts[c] = rows[pl.ds(c, peers, stride=slots), :].astype(BF16)

    def some(i, _):
        at = tile(i, step)
        acc = own_ref[at, :]
        for c in range(slots):
            ends = send_ref[c : c + 1, :] - i * step
            hit = lax.broadcasted_iota(jnp.int32, (step, peers), 0) == ends
            pick = jnp.where(hit, 1.0, 0.0).astype(BF16)
            acc = acc + jnp.dot(pick, parts[c], preferred_element_type=F32)
        sums[at, :] = acc
        return 0

    lax.fori_loop(0, local // step, some, 0)
    lanes = w_self_ref.shape[1]
    w_self_ref[...] = whole_ref[:width, :lanes]
    w_neigh_ref[...] = whole_ref[width:, :lanes]
    bias_ref[...] = jnp.sum(whole_ref[2 * width - 8 :, lanes:], axis=0, keepdims=True)
    for j in range(HUB_MOST):
        to = row(hub_ref[j])
        h = hub_ref[HUB_MOST] + j
        both = whole_ref[row(lax.div(h, 16) * 8 + lax.rem(h, 8)), lanes:]
        late = lax.rem(h, 16) >= 8
        sums[to, :] = sums[to, :] + jnp.where(late, both[:, width:], both[:, :width])

    def close(i, _):
        out_ref[tile(i, step), :] = sums[tile(i, step), :].astype(BF16)
        return 0

    lax.fori_loop(0, local // step, close, 0)


PLANE = 32
MESH = pl.DeviceIdType.MESH


class Places:
    def __init__(self):
        self.count = lax.axis_size("vert")
        self.planes = self.count // PLANE
        self.me = lax.axis_index("vert")
        self.z = lax.div(self.me, PLANE)
        self.p = lax.rem(self.me, PLANE)

    def in_plane(self, i):
        p = lax.rem(self.p + i, PLANE)
        return p, self.z * PLANE + p

    def in_line(self, i):
        z = lax.rem(self.z + i, self.planes)
        return z, z * PLANE + self.p

    def barrier(self, ready):
        entry = pltpu.get_barrier_semaphore()

        def greet_plane(i, _):
            pl.semaphore_signal(entry, device_id=(self.in_plane(i)[1],), device_id_type=MESH)
            return 0

        def greet_line(i, _):
            pl.semaphore_signal(entry, device_id=(self.in_line(i)[1],), device_id_type=MESH)
            return 0

        def vouch(i, _):
            pl.semaphore_signal(ready, device_id=(self.in_line(i)[1],), device_id_type=MESH)
            return 0

        lax.fori_loop(1, PLANE, greet_plane, 0)
        lax.fori_loop(1, self.planes, greet_line, 0)
        pl.semaphore_wait(entry, PLANE + self.planes - 2)
        lax.fori_loop(1, self.planes, vouch, 0)
        pl.semaphore_wait(ready, self.planes - 1)

    def copy(self, src, dst, sems, to):
        return pltpu.make_async_remote_copy(
            src_ref=src,
            dst_ref=dst,
            send_sem=sems.at[0],
            recv_sem=sems.at[1],
            device_id=(to,),
            device_id_type=MESH,
        )

    def all_of(self, ref, sems):
        return self.copy(ref, ref, sems, lax.rem(self.me + 1, self.count))

    def send_blocks(self, src, dst, sems, start, stop):
        def some(k, _):
            t = lax.rem(self.me * 75 + k * 159, self.count)

            @pl.when(t != self.me)
            def _():
                self.copy(src.at[t], dst.at[self.me], sems, t).start()

            return 0

        lax.fori_loop(start, stop, some, 0)


def forward_kernel(sent_ref, hub_ref, halo_ref, hubs_ref, a, b, c, keep, ready):
    here = Places()
    here.barrier(ready)
    own_hub = pltpu.make_async_copy(hub_ref, hubs_ref.at[here.p, here.z], keep.at[0])
    own_hub.start()
    own_halo = pltpu.make_async_copy(sent_ref.at[here.me], halo_ref.at[here.me], keep.at[1])
    own_halo.start()

    def along(i, _):
        here.copy(hub_ref, hubs_ref.at[here.p, here.z], a, here.in_line(i)[1]).start()
        return 0

    lax.fori_loop(1, here.planes, along, 0)
    here.send_blocks(sent_ref, halo_ref, b, 0, here.count // 2)
    own_hub.wait()
    here.all_of(hubs_ref.at[here.p, pl.ds(0, here.planes - 1)], a).wait()

    def across(i, _):
        here.copy(hubs_ref.at[here.p], hubs_ref.at[here.p], c, here.in_plane(i)[1]).start()
        return 0

    lax.fori_loop(1, PLANE, across, 0)
    here.send_blocks(sent_ref, halo_ref, b, here.count // 2, here.count)
    own_halo.wait()
    here.all_of(hubs_ref.at[pl.ds(0, PLANE - 1)], c).wait()
    here.all_of(halo_ref.at[pl.ds(0, here.count - 1)], b).wait()


def backward_kernel(
    back_ref, grads_ref, halo_ref, whole_ref, part_in, parts, part, line, a, b, c, d, keep, ready
):
    here = Places()
    part_in[...] = grads_ref[...].astype(BF16)
    here.barrier(ready)
    kept = [
        pltpu.make_async_copy(back_ref.at[here.me], halo_ref.at[here.me], keep.at[0]),
        pltpu.make_async_copy(part_in.at[here.p], parts.at[here.p], keep.at[1]),
    ]
    for copy in kept:
        copy.start()

    def across(i, _):
        p, to = here.in_plane(i)
        here.copy(part_in.at[p], parts.at[here.p], a, to).start()
        return 0

    lax.fori_loop(1, PLANE, across, 0)
    early, later = here.count * FIRST // 256, here.count * SECOND // 256
    here.send_blocks(back_ref, halo_ref, b, 0, early)
    for copy in kept:
        copy.wait()
    here.all_of(parts.at[pl.ds(0, PLANE - 1)], a).wait()
    part[...] = lax.fori_loop(
        0, PLANE, lambda i, acc: acc + parts[i].astype(F32), jnp.zeros(part.shape, F32)
    )
    here.send_blocks(back_ref, halo_ref, b, early, early + 8)
    kept = pltpu.make_async_copy(part, line.at[here.z], keep.at[0])
    kept.start()

    def along(i, _):
        here.copy(part, line.at[here.z], c, here.in_line(i)[1]).start()
        return 0

    lax.fori_loop(1, here.planes, along, 0)
    here.send_blocks(back_ref, halo_ref, b, early + 8, later)
    kept.wait()
    here.all_of(line.at[pl.ds(0, here.planes - 1)], c).wait()
    whole = line[0]
    for i in range(1, here.planes):
        whole = whole + line[i]
    part[...] = whole
    here.send_blocks(back_ref, halo_ref, b, later, later + 8)
    kept = pltpu.make_async_copy(part, whole_ref.at[here.p], keep.at[0])
    kept.start()

    def spread(i, _):
        here.copy(part, whole_ref.at[here.p], d, here.in_plane(i)[1]).start()
        return 0

    lax.fori_loop(1, PLANE, spread, 0)
    here.send_blocks(back_ref, halo_ref, b, later + 8, here.count)
    kept.wait()
    here.all_of(whole_ref.at[pl.ds(0, PLANE - 1)], d).wait()
    here.all_of(halo_ref.at[pl.ds(0, here.count - 1)], b).wait()


def body(
    feats, w_self, w_neigh, bias, cotangent, send_rows, hub_ids, edge_src, edge_dst, edge_count
):
    local, width = feats.shape
    wide = w_self.shape[1]
    peers = lax.axis_size("vert")
    slots = send_rows.shape[2]
    hub_total = hub_ids.shape[0]
    table_rows = local + peers * slots + hub_total
    params = pltpu.CompilerParams(vmem_limit_bytes=LIMIT)

    send = send_rows[0].T
    planes = peers // PLANE

    sent, own_rows, own_back = pl.pallas_call(
        gather_kernel,
        out_shape=(
            jax.ShapeDtypeStruct((peers, slots, width), BF16),
            jax.ShapeDtypeStruct((HUB_MOST, width), BF16),
            jax.ShapeDtypeStruct((HUB_MOST + 1,), jnp.int32),
        ),
        in_specs=[SMEM, SMEM, VMEM],
        out_specs=(VMEM, VMEM, SMEM),
        scratch_shapes=[
            pltpu.VMEM((local, width), F32),
            pltpu.VMEM((peers * slots, width), F32),
        ],
        compiler_params=params,
        name="gather_sent",
    )(hub_ids, send, feats)
    pair = pltpu.SemaphoreType.DMA((2,))
    halo, hubs = pl.pallas_call(
        forward_kernel,
        out_shape=(
            jax.ShapeDtypeStruct((peers, slots, width), BF16),
            jax.ShapeDtypeStruct((PLANE, planes, HUB_MOST, width), BF16),
        ),
        in_specs=[VMEM, VMEM],
        out_specs=(VMEM, VMEM),
        scratch_shapes=[pair] * 4 + [pltpu.SemaphoreType.REGULAR],
        compiler_params=pltpu.CompilerParams(
            vmem_limit_bytes=LIMIT, collective_id=0, has_side_effects=True
        ),
        name="forward_exchange",
    )(sent, own_rows)
    hubs = hubs.reshape(peers, HUB_MOST, width)

    rows_up = up(table_rows, 64)
    output, own, halo_back, grads = pl.pallas_call(
        layer_kernel,
        out_shape=(
            jax.ShapeDtypeStruct((local, wide), BF16),
            jax.ShapeDtypeStruct((local, width), F32),
            jax.ShapeDtypeStruct((peers, slots, width), BF16),
            jax.ShapeDtypeStruct((2 * width, 2 * wide), F32),
        ),
        in_specs=[SMEM] * 4 + [VMEM] * 8,
        out_specs=(VMEM,) * 4,
        scratch_shapes=[
            pltpu.VMEM((rows_up, width), F32),
            pltpu.VMEM((peers * HUB_MOST, width), F32),
        ]
        + [pltpu.VMEM((local + WINDOW, width), F32)] * 3
        + [pltpu.VMEM((CHUNK, width), F32)] * 2
        + [pltpu.VMEM((rows_up, width), F32)] * STREAMS,
        compiler_params=params,
        name="layer",
    )(
        edge_count, edge_src[0], edge_dst[0], hub_ids, edge_dst.reshape(-1, 128), feats,
        halo, hubs, cotangent, w_self, w_neigh, bias[None, :],
    )

    piece = (2 * width // PLANE, 2 * wide)
    returned, whole = pl.pallas_call(
        backward_kernel,
        out_shape=(
            jax.ShapeDtypeStruct((peers, slots, width), BF16),
            jax.ShapeDtypeStruct((PLANE,) + piece, F32),
        ),
        in_specs=[VMEM] * 2,
        out_specs=(VMEM,) * 2,
        scratch_shapes=[
            pltpu.VMEM((PLANE,) + piece, BF16),
            pltpu.VMEM((PLANE,) + piece, BF16),
            pltpu.VMEM(piece, F32),
            pltpu.VMEM((planes,) + piece, F32),
        ]
        + [pair] * 4
        + [pltpu.SemaphoreType.DMA((2,)), pltpu.SemaphoreType.REGULAR],
        compiler_params=pltpu.CompilerParams(
            vmem_limit_bytes=LIMIT, collective_id=1, has_side_effects=True
        ),
        name="backward_exchange",
    )(halo_back, grads.reshape((PLANE,) + piece))
    whole = whole.reshape(2 * width, 2 * wide)
    grad_feats, grad_w_self, grad_w_neigh, grad_bias = pl.pallas_call(
        final_kernel,
        out_shape=(
            jax.ShapeDtypeStruct((local, width), BF16),
            jax.ShapeDtypeStruct((width, wide), F32),
            jax.ShapeDtypeStruct((width, wide), F32),
            jax.ShapeDtypeStruct((1, wide), F32),
        ),
        in_specs=[SMEM] + [VMEM] * 4,
        out_specs=(VMEM,) * 4,
        scratch_shapes=[
            pltpu.VMEM((peers * slots, width), F32),
            pltpu.VMEM((slots, peers, width), BF16),
            pltpu.VMEM((up(local + 1, 8), width), F32),
        ],
        compiler_params=params,
        name="final",
    )(own_back, send, own, returned, whole)
    return (output, grad_feats, grad_w_self, grad_w_neigh, grad_bias[0])


def solution(mesh):
    in_specs = (
        P("vert", None),
        P(),
        P(),
        P(),
        P("vert", None),
        P("vert", None, None),
        P(),
        P("vert", None),
        P("vert", None),
        P("vert"),
    )
    out_specs = (P("vert", None), P("vert", None), P(), P(), P())
    return jax.shard_map(body, mesh=mesh, in_specs=in_specs, out_specs=out_specs, check_vma=False)
```
